128 devices in a mesh: dp: 8 (over y_lo, x), tensor: 16 (over z, y_hi, core).
Axes of the slice: x: 4, y: 4 (y_hi: 2, y_lo: 2; y = y_hi * 2 + y_lo), z: 4, core: 2. Of those that a mesh axis runs over, the one named last changes fastest.
Arguments:
- tokens: bfloat16 [8192, 2048], P(('dp', 'tensor')), may hold values from -12 to 12
- targets: bfloat16 [8192, 2048], P(('dp', 'tensor')), may hold values from -6 to 6
- learner_gain: float32 [2048], replicated, may hold values from 0.1 to 1.9
- learner_gate: bfloat16 [2048, 8192], P(None, 'tensor'), may hold values from -0.125 to 0.125
- learner_up: bfloat16 [2048, 8192], P(None, 'tensor'), may hold values from -0.125 to 0.125
- learner_down: bfloat16 [8192, 2048], P('tensor'), may hold values from -0.0625 to 0.0625
- frozen_gain: float32 [2048], replicated, may hold values from 0.1 to 1.9
- frozen_gate: bfloat16 [2048, 8192], P(None, 'tensor'), may hold values from -0.125 to 0.125
- frozen_up: bfloat16 [2048, 8192], P(None, 'tensor'), may hold values from -0.125 to 0.125
- frozen_down: bfloat16 [8192, 2048], P('tensor'), may hold values from -0.0625 to 0.0625
Outputs:
- scores: float32 [8192], P(('dp', 'tensor'))
- grad_tokens: bfloat16 [8192, 2048], P(('dp', 'tensor'))
- grad_gain: float32 [2048], replicated
- grad_gate: float32 [2048, 8192], P('dp', 'tensor')
- grad_up: float32 [2048, 8192], P('dp', 'tensor')
- grad_down: float32 [8192, 2048], P('tensor', 'dp')
The draws below stay inside these ranges and needn't reach their ends.
All inputs are finite; a program needn't handle non-finite values.
Results may differ from the reference program's by a relative error of at most 0.0096.
Values may be sent and summed in bfloat16 or wider, within the bound.
A program may use at most 128 MiB of HBM per device.

```python
import math
import jax
import jax.numpy as jnp
from jax import lax

D = 2048
FF = 8192
TOKENS = 8192


def draw_tokens(key, part):
    first, second = jax.random.split(jax.random.fold_in(key, 11))
    base = jnp.clip(jax.random.normal(first, (TOKENS, D), jnp.float32), -4.0, 4.0)
    scale = jnp.exp(jax.random.uniform(second, (TOKENS, 1), jnp.float32, math.log(0.3), math.log(3.0)))
    return (base * scale).astype(jnp.bfloat16)


def level_of(rng, dims, pieces, least, largest):
    loudness = 1.0
    for position, shards_of in pieces:
        steps = jax.random.uniform(jax.random.fold_in(jax.random.fold_in(rng, 6), position), (shards_of,), jnp.float32, least / len(pieces), largest / len(pieces))
        loudness = loudness * jnp.repeat(jnp.exp(steps), dims[position] // shards_of).reshape((-1,) + (1,) * (len(dims) - 1 - position))
    return loudness


def noise(own_key, shape, deviation, most, shards=(), held_as=jnp.bfloat16):
    values = jax.random.normal(own_key, shape, jnp.float32) * deviation
    if len(shards) > 0:
        values = level_of(own_key, shape, shards, -0.22, 0.18) * values
    return jnp.clip(values, min=-most, max=most).astype(held_as)


def setup_inputs(seed: int = 0) -> dict:
    splits = jax.random.split(jax.random.key(seed), 11)
    return {
        "tokens": draw_tokens(jax.random.fold_in(splits[10], 71), 0),
        "targets": noise(splits[1], (TOKENS, D), 1.0, 6.0, ((0, 128),)),
        "learner_gain": jnp.clip(1.0 + 0.18 * jax.random.normal(splits[2], (D,), jnp.float32), 0.1, 1.9),
        "learner_gate": noise(splits[3], (D, FF), D ** -0.5, 0.125, ((1, 16),)),
        "learner_up": noise(splits[4], (D, FF), D ** -0.5, 0.125, ((1, 16),)),
        "learner_down": noise(splits[5], (FF, D), FF ** -0.5, 0.0625, ((0, 16),)),
        "frozen_gain": jnp.clip(1.0 + 0.18 * jax.random.normal(splits[6], (D,), jnp.float32), 0.1, 1.9),
        "frozen_gate": noise(splits[7], (D, FF), D ** -0.5, 0.125, ((1, 16),)),
        "frozen_up": noise(splits[8], (D, FF), D ** -0.5, 0.125, ((1, 16),)),
        "frozen_down": noise(splits[9], (FF, D), FF ** -0.5, 0.0625, ((0, 16),)),
    }


def feed_forward(normed, w_gate, w_up, w_down):
    gate_pre = jnp.dot(normed, w_gate, preferred_element_type=jnp.float32)
    up_pre = jnp.dot(normed, w_up, preferred_element_type=jnp.float32)
    hidden = (jax.nn.silu(gate_pre) * up_pre).astype(jnp.bfloat16)
    output = jnp.dot(hidden, w_down, preferred_element_type=jnp.float32)
    return (gate_pre, up_pre, hidden, output)

def reference(tokens, targets, learner_gain, learner_gate, learner_up, learner_down, frozen_gain, frozen_gate, frozen_up, frozen_down):
    xfloat = tokens.astype(jnp.float32)
    inv_rms = lax.rsqrt(lax.optimization_barrier(jnp.mean(xfloat * xfloat, axis=-1, keepdims=True)) + 1e-05)
    normed = (xfloat * inv_rms * learner_gain).astype(jnp.bfloat16)
    frozen_normed = (xfloat * inv_rms * frozen_gain).astype(jnp.bfloat16)
    gate_pre, up_pre, hidden, learned = feed_forward(normed, learner_gate, learner_up, learner_down)
    frozen_out = feed_forward(frozen_normed, frozen_gate, frozen_up, frozen_down)[3]
    goal = targets.astype(jnp.float32)
    root = math.sqrt(tokens.shape[1])
    miss = learned - goal
    frozen_miss = frozen_out - goal
    learner_loss = 0.5 * lax.optimization_barrier(jnp.sum(miss * miss, axis=-1)) / root
    frozen_loss = 0.5 * lax.optimization_barrier(jnp.sum(frozen_miss * frozen_miss, axis=-1)) / root
    scores = learner_loss - frozen_loss
    weight = jax.nn.sigmoid(scores)
    out_grad = (weight[:, None] * miss / root).astype(jnp.bfloat16)
    grad_down = jnp.dot(hidden.T, out_grad, preferred_element_type=jnp.float32)
    hidden_grad = jnp.dot(out_grad, learner_down.T, preferred_element_type=jnp.float32)
    sigma = jax.nn.sigmoid(gate_pre)
    gate_grad = (hidden_grad * up_pre * sigma * (1.0 + gate_pre * (1.0 - sigma))).astype(jnp.bfloat16)
    up_grad = (hidden_grad * gate_pre * sigma).astype(jnp.bfloat16)
    grad_gate = jnp.dot(normed.T, gate_grad, preferred_element_type=jnp.float32)
    grad_up = jnp.dot(normed.T, up_grad, preferred_element_type=jnp.float32)
    normed_grad = jnp.dot(gate_grad, learner_gate.T, preferred_element_type=jnp.float32) + jnp.dot(up_grad, learner_up.T, preferred_element_type=jnp.float32)
    grad_gain = lax.optimization_barrier(jnp.sum(normed_grad * xfloat * inv_rms, axis=0))
    scaled = learner_gain * normed_grad
    cubed = inv_rms * inv_rms * inv_rms
    grad_tokens = (inv_rms * scaled - xfloat * cubed * lax.optimization_barrier(jnp.mean(scaled * xfloat, axis=-1, keepdims=True))).astype(jnp.bfloat16)
    return (scores, grad_tokens, grad_gain, grad_gate, grad_up, grad_down)
```

```python
import functools
import math

import jax
import jax.numpy as jnp
from jax import lax
from jax.experimental import pallas as pl
from jax.experimental.pallas import tpu as pltpu
from jax.sharding import PartitionSpec as P

F32 = jnp.float32
BF16 = jnp.bfloat16
MESH = pl.DeviceIdType.MESH
VMEM_LIMIT = 66_000_000
ROWS = 16


class Wires:
    def __init__(self, send_sems, recv_sems):
        self.send_sems, self.recv_sems, self.sent = send_sems, recv_sems, []

    def send(self, src, dst, out, into, device):
        copy = pltpu.make_async_remote_copy(
            src_ref=src,
            dst_ref=dst,
            send_sem=self.send_sems.at[out],
            recv_sem=self.recv_sems.at[into],
            device_id=device,
            device_id_type=MESH,
        )
        copy.start()
        self.sent.append(copy)

    def got(self, ref, into, device):
        pltpu.make_async_remote_copy(
            src_ref=ref,
            dst_ref=ref,
            send_sem=self.send_sems.at[0],
            recv_sem=self.recv_sems.at[into],
            device_id=device,
            device_id_type=MESH,
        ).wait_recv()

    def drain(self):
        for copy in self.sent:
            copy.wait_send()


class Seat:
    def __init__(self):
        t = lax.axis_index("tensor")
        self.t = t
        self.z, self.y, self.c = t // 4, (t // 2) % 2, t % 2
        self.zp, self.zm, self.zf = (self.z + 1) % 4, (self.z + 3) % 4, (self.z + 2) % 4
        self.o, self.s = 1 - self.y, 1 - self.c

    def dev(self, z, y, c):
        return {"tensor": z * 4 + y * 2 + c}

    def pairs(self, i):
        yy = (self.y + i // 2) % 2
        a, b = (self.z + i % 2) % 4, (self.z + 3 - i % 2) % 4
        return a * 2 + yy, b * 2 + yy


def meet(devices):
    barrier = pltpu.get_barrier_semaphore()
    for device in devices:
        pl.semaphore_signal(barrier, inc=1, device_id=device, device_id_type=MESH)
    pl.semaphore_wait(barrier, len(devices))


class Gather:
    def __init__(self, seat, own, full, send_sems, recv_sems):
        self.s, self.own, self.full = seat, own, full
        self.w = Wires(send_sems, recv_sems)
        self.half = own.shape[0] // 2

    def blk(self, z, y, c, part=None):
        ref = self.full.at[z * 2 + y, c]
        return ref if part is None else ref.at[pl.ds(part * self.half, self.half)]

    def pass_on(self, z, y, out, into, device, part=None):
        b = self.blk(z, y, self.s.c, part)
        self.w.send(b, b, out, into, device)

    def got(self, z, y, c, into, part=None):
        s = self.s
        self.w.got(self.blk(z, y, c, part), into, s.dev(s.z, s.y, s.s))

    def start(self):
        s = self.s
        home = self.blk(s.z, s.y, s.c)
        self.w.send(self.own, home, 0, 0, s.dev(s.zp, s.y, s.c))
        self.w.send(self.own, home, 1, 1, s.dev(s.zm, s.y, s.c))
        self.w.send(self.own, home, 2, 2, s.dev(s.z, s.o, s.c))
        self.w.send(self.own, home, 3, 9, s.dev(s.z, s.y, s.s))
        self.full[s.z * 2 + s.y, s.c] = self.own[...]

    def step(self, i):
        s = self.s
        up, down, sib = s.dev(s.zp, s.y, s.c), s.dev(s.zm, s.y, s.c), s.dev(s.z, s.y, s.s)
        if i == 0:
            self.got(s.zm, s.y, s.c, 0)
            self.pass_on(s.zm, s.y, 4, 5, up, 0)
            self.pass_on(s.zm, s.y, 6, 10, sib)
            self.got(s.zp, s.y, s.c, 1)
            self.pass_on(s.zp, s.y, 5, 6, down, 1)
            self.pass_on(s.zp, s.y, 7, 11, sib)
            self.got(s.z, s.y, s.s, 9)
            self.got(s.zm, s.y, s.s, 10)
        if i == 1:
            self.got(s.z, s.o, s.c, 2)
            self.pass_on(s.z, s.o, 8, 3, up)
            self.pass_on(s.z, s.o, 9, 4, down)
            self.pass_on(s.z, s.o, 10, 12, sib)
            self.got(s.zf, s.y, s.c, 5, 0)
            self.got(s.zf, s.y, s.c, 6, 1)
            self.pass_on(s.zf, s.y, 15, 15, sib)
            self.got(s.zp, s.y, s.s, 11)
            self.got(s.zf, s.y, s.s, 15)
        if i == 2:
            self.got(s.zm, s.o, s.c, 3)
            self.pass_on(s.zm, s.o, 11, 7, up, 0)
            self.pass_on(s.zm, s.o, 13, 13, sib)
            self.got(s.zp, s.o, s.c, 4)
            self.pass_on(s.zp, s.o, 12, 8, down, 1)
            self.pass_on(s.zp, s.o, 14, 14, sib)
            self.got(s.z, s.o, s.s, 12)
            self.got(s.zm, s.o, s.s, 13)
        if i == 3:
            self.got(s.zf, s.o, s.c, 7, 0)
            self.got(s.zf, s.o, s.c, 8, 1)
            self.pass_on(s.zf, s.o, 16, 16, sib)
            self.got(s.zp, s.o, s.s, 14)
            self.got(s.zf, s.o, s.s, 16)


def fold(dst, refs, lo=0, hi=None):
    hi = dst.shape[0] if hi is None else hi

    def rows(k, carry):
        at = pl.ds(pl.multiple_of(lo + k * ROWS, ROWS), ROWS)
        total = refs[0][at].astype(F32)
        for ref in refs[1:]:
            total = total + ref[at].astype(F32)
        dst[at] = total.astype(dst.dtype)
        return carry

    lax.fori_loop(0, (hi - lo) // ROWS, rows, 0)


class RingSum:
    def __init__(self, block, dev, ring, row, slots, last, send_sems, recv_sems, base):
        self.block, self.dev, self.slots, self.last, self.base = block, dev, slots, last, base
        self.r, self.y, self.o = ring, row, 1 - row
        self.rp, self.rm, self.rf = (ring + 1) % 4, (ring + 3) % 4, (ring + 2) % 4
        self.w = Wires(send_sems, recv_sems)

    def out(self, r, y, slot, to, more=()):
        refs = self.block(r, y)
        if len(refs) + len(more) > 1:
            fold(refs[0], refs + [self.slots.at[k] for k in more])
        self.w.send(refs[0], self.slots.at[slot], self.base + slot, self.base + slot, to)

    def got(self, slot):
        self.w.got(self.slots.at[slot], self.base + slot, self.dev(self.rp, self.y))

    def stage1(self):
        up, down = self.dev(self.rp, self.y), self.dev(self.rm, self.y)
        self.out(self.rf, 0, 0, up)
        self.out(self.rf, 1, 1, down)
        self.out(self.rp, 1, 3, up)
        self.out(self.rm, 0, 4, down)

    def stage2(self):
        self.got(0)
        self.out(self.rp, 0, 2, self.dev(self.rp, self.y), (0,))
        self.got(1)
        self.out(self.rm, 1, 5, self.dev(self.rm, self.y), (1,))

    def stage3(self):
        for k in (3, 4, 2, 5):
            self.got(k)
        refs = self.block(self.r, self.o)
        fold(refs[0], refs + [self.slots.at[2 + self.o], self.slots.at[4 + self.o]])
        self.w.send(refs[0], self.last, self.base + 6, self.base + 6, self.dev(self.r, self.o))

    def stage4(self):
        self.w.got(self.last, self.base + 6, self.dev(self.r, self.o))
        refs = self.block(self.r, self.y)
        return refs + [self.slots.at[2 + self.y], self.slots.at[4 + self.y], self.last]


class GroupSum(RingSum):
    def __init__(self, seat, partial, paired, slots, last, send_sems, recv_sems):
        self.s, self.partial, self.paired = seat, partial, paired
        super().__init__(
            lambda z, y: [partial.at[z * 2 + y, seat.c], paired.at[z * 2 + y]],
            lambda z, y: seat.dev(z, y, seat.c),
            seat.z,
            seat.y,
            slots,
            last,
            send_sems,
            recv_sems,
            8,
        )

    def pair_send(self, i):
        s = self.s
        for j, p in enumerate(s.pairs(i)):
            k = 2 * i + j
            self.w.send(self.partial.at[p, s.s], self.paired.at[p], k, k, s.dev(s.z, s.y, s.s))

    def pair_got(self):
        s = self.s
        for i in range(4):
            for j, p in enumerate(s.pairs(i)):
                self.w.got(self.paired.at[p], 2 * i + j, s.dev(s.z, s.y, s.s))


def total_of(refs, at):
    total = refs[0][at].astype(F32)
    for ref in refs[1:]:
        total = total + ref[at].astype(F32)
    return total


def sigmoid(v):
    return 1.0 / (1.0 + jnp.exp(-v))


def dot(a, b):
    return jnp.dot(a, b, preferred_element_type=F32)


def dot_t(a, b):
    return lax.dot_general(a, b, (((1,), (1,)), ((), ())), preferred_element_type=F32)


def tile(j, size):
    return pl.ds(pl.multiple_of(j * size, size), size)


def rows_of(ref, p1, p2):
    width = ref.shape[-1]
    return jnp.concatenate([ref[p1].reshape(-1, width), ref[p2].reshape(-1, width)], axis=0)


def forward_kernel(
    tokens, targets, lgain, fgain, wg, wu, wd, fg, fu, fd,
    scores, ograd, normed_out, gate_out, up_out, hid_out,
    full, normed, fnormed, gate, up, hid_t, hid, lpart, fpart,
    lpaired, fpaired, lslots, fslots, llast, flast,
    vwg, vwu, vwd, vfg, vfu, vfd,
    load_sems, gsend, grecv, lsend, lrecv, fsend, frecv,
):
    seat = Seat()
    s = seat
    width = tokens.shape[1]
    hidden = vwg.shape[1]
    block = tokens.shape[0]
    loads = [
        pltpu.make_async_copy(src, dst, load_sems.at[k])
        for k, (src, dst) in enumerate(
            ((fg, vfg), (fu, vfu), (fd, vfd), (wg, vwg), (wu, vwu), (wd, vwd))
        )
    ]
    for copy in loads:
        copy.start()
    meet([s.dev(s.z, s.y, s.s), s.dev(s.zp, s.y, s.c), s.dev(s.zm, s.y, s.c), s.dev(s.z, s.o, s.c)])
    gather = Gather(s, tokens, full, gsend, grecv)
    learner = GroupSum(s, lpart, lpaired, lslots, llast, lsend, lrecv)
    frozen = GroupSum(s, fpart, fpaired, fslots, flast, fsend, frecv)
    gather.start()

    def normalize(i):
        for j, p in enumerate(s.pairs(i)):
            for core in range(2):

                def rows(k, carry, p=p, core=core, j=j):
                    at = pl.ds(pl.multiple_of(k * ROWS, ROWS), ROWS)
                    x = full[p, core, at].astype(F32)
                    unit = x * lax.rsqrt(jnp.mean(x * x, axis=-1, keepdims=True) + 1e-05)
                    normed[p, core, at] = (unit * lgain[...]).astype(BF16)
                    fnormed[j, core, at] = (unit * fgain[...]).astype(BF16)
                    return carry

                lax.fori_loop(0, block // ROWS, rows, 0)

    def put(part, i, cols, value):
        p1, p2 = s.pairs(i)
        value = value.astype(BF16).reshape(2, 2, block, value.shape[-1])
        part[p1, :, :, cols] = value[0]
        part[p2, :, :, cols] = value[1]

    nt, wt = min(256, hidden), min(512, width)

    def run_frozen(i):
        def cols(j, carry):
            at = tile(j, nt)
            lhs = rows_of(fnormed, 0, 1)
            g, u = dot(lhs, vfg[:, at]), dot(lhs, vfu[:, at])
            hid[:, at] = (g * sigmoid(g) * u).astype(BF16)
            return carry

        lax.fori_loop(0, hidden // nt, cols, 0)

        def outs(j, carry):
            at = tile(j, wt)
            put(fpart, i, at, dot(hid[...], vfd[:, at]))
            return carry

        lax.fori_loop(0, width // wt, outs, 0)

    def run_learner(i, carry):
        p1, p2 = s.pairs(i)
        n = 2 * block

        def cols(j, carry):
            at = tile(j, nt)
            lhs = rows_of(normed, p1, p2)
            g, u = dot(lhs, vwg[:, at]), dot(lhs, vwu[:, at])
            gate[p1, :, at], gate[p2, :, at] = g[:n], g[n:]
            up[p1, :, at], up[p2, :, at] = u[:n], u[n:]
            h = g * sigmoid(g) * u
            hid[:, at] = h.astype(BF16)
            ht = h.T.astype(BF16)
            hid_t[at, tile(p1, n)] = ht[:, :n]
            hid_t[at, tile(p2, n)] = ht[:, n:]
            return carry

        lax.fori_loop(0, hidden // nt, cols, 0)

        def outs(j, carry):
            at = tile(j, wt)
            put(lpart, i, at, dot(hid[...], vwd[:, at]))
            return carry

        lax.fori_loop(0, width // wt, outs, 0)
        return carry

    for i in range(4):
        gather.step(i)
        normalize(i)
        if i == 0:
            for copy in loads[:3]:
                copy.wait()
        run_frozen(i)
        frozen.pair_send(i)
    stores = [pltpu.make_async_copy(normed, normed_out, load_sems.at[6])]
    stores[0].start()
    for copy in loads[3:]:
        copy.wait()
    frozen.pair_got()
    frozen.stage1()
    lax.fori_loop(0, 2, run_learner, 0)
    learner.pair_send(0)
    learner.pair_send(1)
    frozen.stage2()
    lax.fori_loop(2, 4, run_learner, 0)
    learner.pair_send(2)
    learner.pair_send(3)
    for k, (src, dst) in enumerate(((gate, gate_out), (up, up_out), (hid_t, hid_out))):
        stores.append(pltpu.make_async_copy(src, dst, load_sems.at[7 + k]))
        stores[-1].start()
    learner.pair_got()
    learner.stage1()
    frozen.stage3()
    learner.stage2()
    learner.stage3()
    frefs = frozen.stage4()
    lrefs = learner.stage4()
    root = math.sqrt(width)

    def rows(k, carry):
        at = pl.ds(pl.multiple_of(k * ROWS, ROWS), ROWS)
        goal = targets[at].astype(F32)
        fmiss = total_of(frefs, at) - goal
        frozen_loss = 0.5 * jnp.sum(fmiss * fmiss, axis=-1, keepdims=True) / root
        miss = total_of(lrefs, at) - goal
        learner_loss = 0.5 * jnp.sum(miss * miss, axis=-1, keepdims=True) / root
        score = learner_loss - frozen_loss
        scores[at] = score
        ograd[at] = (sigmoid(score) * miss / root).astype(BF16)
        return carry

    lax.fori_loop(0, block // ROWS, rows, 0)
    for copy in stores:
        copy.wait()
    for part in (gather, learner, frozen):
        part.w.drain()


def backward_kernel(
    own, tokens, lgain, wg, wu, wd, normed_in, gate_in, up_in, hid_in,
    grad_tokens, grad_gain, out_gate, out_up, out_down,
    full, normed, gate, up, hid_t, gg, ug, ggt, ugt, terms,
    part, paired, slots, last, gslots, glast, uslots, ulast, dslots, dfar, dlast,
    gain_acc, gain_t, gain_d, vwg, vwu, vwd,
    load_sems, ssend, srecv, nsend, nrecv, qsend, qrecv, dsend, drecv, tsend, trecv, psend, precv,
):
    seat = Seat()
    s = seat
    d = lax.axis_index("dp")
    x, yl = d % 4, d // 4
    xp, xm, xf = (x + 1) % 4, (x + 3) % 4, (x + 2) % 4
    block, width = tokens.shape
    hidden = vwg.shape[1]
    cut = width // 8
    loads = [
        pltpu.make_async_copy(src, dst, load_sems.at[k])
        for k, (src, dst) in enumerate(
            (
                (wd, vwd), (gate_in, gate), (up_in, up), (normed_in, normed),
                (hid_in, hid_t), (wg, vwg), (wu, vwu),
            )
        )
    ]
    for copy in loads:
        copy.start()
    meet(
        [{"tensor": (s.t + r) % 16} for r in range(1, 16)]
        + [{"dp": (d + r) % 8} for r in range(1, 8)]
    )
    gather = Gather(s, own, full, ssend, srecv)
    gather.start()
    summed = GroupSum(s, part, paired, slots, last, nsend, nrecv)
    gate_sum = RingSum(
        lambda xx, yy: [terms.at[0, yy * 4 + xx]], lambda xx, yy: {"dp": yy * 4 + xx},
        x, yl, gslots, glast, qsend, qrecv, 0,
    )
    up_sum = RingSum(
        lambda xx, yy: [terms.at[1, yy * 4 + xx]], lambda xx, yy: {"dp": yy * 4 + xx},
        x, yl, uslots, ulast, qsend, qrecv, 7,
    )
    down_w = Wires(dsend, drecv)
    n = 2 * block
    nt, wt = min(256, hidden), min(512, width)

    def back(i):
        p1, p2 = s.pairs(i)

        def cols(j, carry):
            at = tile(j, nt)
            hg = dot_t(rows_of(full, p1, p2), vwd[at, :])
            g = jnp.concatenate([gate[p1, :, at], gate[p2, :, at]], axis=0)
            u = jnp.concatenate([up[p1, :, at], up[p2, :, at]], axis=0)
            sigma = sigmoid(g)
            side = hg * sigma
            ggrad = side * u * (1.0 + g * (1.0 - sigma))
            ugrad = side * g
            for value, plain, flipped in ((ggrad, gg, ggt), (ugrad, ug, ugt)):
                low = value.astype(BF16)
                plain[p1, :, at], plain[p2, :, at] = low[:n], low[n:]
                turned = value.T.astype(BF16)
                flipped[at, tile(p1, n)] = turned[:, :n]
                flipped[at, tile(p2, n)] = turned[:, n:]
            return carry

        lax.fori_loop(0, hidden // nt, cols, 0)

    for i in range(4):
        gather.step(i)
        if i == 0:
            for copy in loads[:3]:
                copy.wait()
        back(i)
    for copy in loads[3:]:
        copy.wait()

    def term(q, lhs, rhs, dd):
        at = tile(dd, cut)
        terms[q, dd] = dot(lhs[...], rhs[:, :, :, at].reshape(16 * block, cut)).astype(BF16)

    def ring_terms(q, lhs, lo, hi):
        def one(k, code):
            term(q, lhs, normed, (k % 2) * 4 + (x + code % 4) % 4)
            return code // 4

        lax.fori_loop(lo, hi, one, jnp.int32(3450 // 4**lo))

    def down_terms(row):
        def one(k, carry):
            term(2, hid_t, full, row * 4 + k)
            return carry

        lax.fori_loop(0, 4, one, 0)

    def normed_part(i, carry):
        p1, p2 = s.pairs(i)

        def outs(j, carry):
            at = tile(j, wt)
            value = dot_t(rows_of(gg, p1, p2), vwg[at, :]) + dot_t(rows_of(ug, p1, p2), vwu[at, :])
            value = value.astype(BF16).reshape(2, 2, block, wt)
            part[p1, :, :, at] = value[0]
            part[p2, :, :, at] = value[1]
            return carry

        lax.fori_loop(0, width // wt, outs, 0)
        return carry

    ring_terms(0, ggt, 0, 4)
    gate_sum.stage1()
    down_terms(1 - yl)
    across = {"dp": (1 - yl) * 4 + x}
    to_up, to_down = {"dp": yl * 4 + xp}, {"dp": yl * 4 + xm}
    for k in range(4):
        down_w.send(terms.at[2, (1 - yl) * 4 + k], dslots.at[k], k, k, across)
    ring_terms(0, ggt, 4, 8)
    ring_terms(1, ugt, 0, 4)
    up_sum.stage1()
    ring_terms(1, ugt, 4, 8)
    gate_sum.stage2()
    down_terms(yl)
    lax.fori_loop(0, 2, normed_part, 0)
    summed.pair_send(0)
    summed.pair_send(1)
    lax.fori_loop(2, 4, normed_part, 0)
    summed.pair_send(2)
    summed.pair_send(3)
    summed.pair_got()
    summed.stage1()
    for k in range(4):
        down_w.got(dslots.at[k], k, across)
    half = hidden // 2

    def mine(xx):
        return terms.at[2, yl * 4 + xx]

    def piece(ref, h):
        return ref.at[pl.ds(h * half, half)]

    fold(mine(xf), [mine(xf), dslots.at[xf]])
    down_w.send(piece(mine(xf), 0), dfar.at[0], 4, 4, to_up)
    down_w.send(piece(mine(xf), 1), dfar.at[1], 5, 5, to_down)
    fold(mine(xp), [mine(xp), dslots.at[xp]])
    down_w.send(piece(mine(xp), 1), piece(dlast.at[0], 1), 6, 6, to_up)
    fold(mine(xm), [mine(xm), dslots.at[xm]])
    down_w.send(piece(mine(xm), 0), piece(dlast.at[1], 0), 7, 7, to_down)
    up_sum.stage2()
    summed.stage2()
    down_w.got(dfar.at[0], 4, to_up)
    fold(piece(mine(xp), 0), [piece(mine(xp), 0), dfar.at[0]])
    down_w.send(piece(mine(xp), 0), piece(dlast.at[0], 0), 8, 8, to_up)
    down_w.got(dfar.at[1], 5, to_up)
    fold(piece(mine(xm), 1), [piece(mine(xm), 1), dfar.at[1]])
    down_w.send(piece(mine(xm), 1), piece(dlast.at[1], 1), 9, 9, to_down)
    summed.stage3()
    gate_sum.stage3()
    nrefs = summed.stage4()
    gain_acc[...] = jnp.zeros_like(gain_acc)

    def rows(k, carry):
        at = pl.ds(pl.multiple_of(k * ROWS, ROWS), ROWS)
        v = tokens[at].astype(F32)
        inv = lax.rsqrt(jnp.mean(v * v, axis=-1, keepdims=True) + 1e-05)
        ng = total_of(nrefs, at)
        scaled = ng * lgain[...]
        mid = jnp.mean(scaled * v, axis=-1, keepdims=True)
        grad_tokens[at] = (inv * scaled - v * (inv * inv * inv * mid)).astype(BF16)
        term = ng * v * inv
        gain_acc[...] += term[:8] + term[8:]
        return carry

    lax.fori_loop(0, block // ROWS, rows, 0)
    gain_t[s.t] = jnp.sum(gain_acc[...], axis=0, keepdims=True)
    tw, pw = Wires(tsend, trecv), Wires(psend, precv)
    for r in range(1, 16):
        tw.send(gain_t.at[s.t], gain_t.at[s.t], r - 1, r - 1, {"tensor": (s.t + r) % 16})
    up_sum.stage3()

    def finish(out, refs):
        def rows(k, carry):
            at = pl.ds(pl.multiple_of(k * ROWS, ROWS), ROWS)
            out[at] = total_of(refs, at)
            return carry

        lax.fori_loop(0, hidden // ROWS, rows, 0)

    finish(out_gate, gate_sum.stage4())
    for r in range(1, 16):
        tw.got(gain_t.at[(s.t + 16 - r) % 16], r - 1, {"tensor": (s.t + 1) % 16})
    gain_d[d] = jnp.sum(gain_t[...], axis=0)
    for r in range(1, 8):
        pw.send(gain_d.at[d], gain_d.at[d], r - 1, r - 1, {"dp": (d + r) % 8})
    for h in (1, 0):
        for k in (0, 1):
            at = ((8, 7), (6, 9))[h][k]
            down_w.got(piece(dlast.at[k], h), at, to_up)
    finish(out_down, [mine(x), dslots.at[x], dlast.at[0], dlast.at[1]])
    finish(out_up, up_sum.stage4())
    for r in range(1, 8):
        pw.got(gain_d.at[(d + 8 - r) % 8], r - 1, {"dp": (d + 1) % 8})
    grad_gain[...] = jnp.sum(gain_d[...], axis=0)
    for wires in (gather.w, summed.w, gate_sum.w, up_sum.w, down_w, tw, pw):
        wires.drain()


def local(
    tokens, targets, learner_gain, learner_gate, learner_up, learner_down,
    frozen_gain, frozen_gate, frozen_up, frozen_down,
):
    block, width = tokens.shape
    hidden = learner_gate.shape[1]
    dma = pltpu.SemaphoreType.DMA
    here = pl.BlockSpec(memory_space=pltpu.VMEM)
    away = pl.BlockSpec(memory_space=pl.ANY)
    shape = jax.ShapeDtypeStruct
    params = functools.partial(
        pltpu.CompilerParams, has_side_effects=True, vmem_limit_bytes=VMEM_LIMIT
    )
    gain = learner_gain.reshape(1, width)
    group = 16 * block
    up_w, down_w = pltpu.VMEM((width, hidden), BF16), pltpu.VMEM((hidden, width), BF16)
    sums = [
        pltpu.VMEM((8, block, width), BF16),
        pltpu.VMEM((6, block, width), BF16),
        pltpu.VMEM((block, width), BF16),
    ]
    blocks = pltpu.VMEM((8, 2, block, width), BF16)
    pre = pltpu.VMEM((8, 2 * block, hidden), F32)
    scores, ograd, normed, gate, up, hid_t = pl.pallas_call(
        forward_kernel,
        out_shape=(
            shape((block, 1), F32),
            shape((block, width), BF16),
            shape((8, 2, block, width), BF16),
            shape((8, 2 * block, hidden), F32),
            shape((8, 2 * block, hidden), F32),
            shape((hidden, group), BF16),
        ),
        in_specs=[here] * 4 + [away] * 6,
        out_specs=[here] * 2 + [away] * 4,
        scratch_shapes=[
            blocks,
            blocks,
            pltpu.VMEM((2, 2, block, width), BF16),
            pre,
            pre,
            pltpu.VMEM((hidden, group), BF16),
            pltpu.VMEM((4 * block, hidden), BF16),
            blocks,
            blocks,
            sums[0],
            sums[0],
            sums[1],
            sums[1],
            sums[2],
            sums[2],
            up_w,
            up_w,
            down_w,
            up_w,
            up_w,
            down_w,
            dma((10,)),
            dma((17,)),
            dma((17,)),
            dma((15,)),
            dma((15,)),
            dma((15,)),
            dma((15,)),
        ],
        compiler_params=params(collective_id=1),
        name="forward",
    )(
        tokens, targets, gain, frozen_gain.reshape(1, width), learner_gate, learner_up,
        learner_down, frozen_gate, frozen_up, frozen_down,
    )
    cut = width // 8
    mine = pltpu.VMEM((hidden, cut), BF16)
    grad = shape((hidden, cut), F32)
    flat = pltpu.VMEM((8, 2 * block, hidden), BF16)
    grad_tokens, grad_gain, grad_gate, grad_up, grad_down = pl.pallas_call(
        backward_kernel,
        out_shape=(shape((block, width), BF16), shape((1, width), F32), grad, grad, grad),
        in_specs=[here] * 3 + [away] * 7,
        out_specs=[here] * 5,
        scratch_shapes=[
            blocks,
            blocks,
            pre,
            pre,
            pltpu.VMEM((hidden, group), BF16),
            flat,
            flat,
            pltpu.VMEM((hidden, group), BF16),
            pltpu.VMEM((hidden, group), BF16),
            pltpu.VMEM((3, 8, hidden, cut), BF16),
            blocks,
            sums[0],
            sums[1],
            sums[2],
            pltpu.VMEM((6, hidden, cut), BF16),
            mine,
            pltpu.VMEM((6, hidden, cut), BF16),
            mine,
            pltpu.VMEM((4, hidden, cut), BF16),
            pltpu.VMEM((2, hidden // 2, cut), BF16),
            pltpu.VMEM((2, hidden, cut), BF16),
            pltpu.VMEM((8, width), F32),
            pltpu.VMEM((16, 1, width), F32),
            pltpu.VMEM((8, 1, width), F32),
            up_w,
            up_w,
            down_w,
            dma((7,)),
            dma((17,)),
            dma((17,)),
            dma((15,)),
            dma((15,)),
            dma((14,)),
            dma((14,)),
            dma((10,)),
            dma((10,)),
            dma((15,)),
            dma((15,)),
            dma((7,)),
            dma((7,)),
        ],
        compiler_params=params(collective_id=2),
        name="backward",
    )(ograd, tokens, gain, learner_gate, learner_up, learner_down, normed, gate, up, hid_t)
    return (
        scores.reshape(block),
        grad_tokens,
        grad_gain.reshape(width),
        grad_gate.T,
        grad_up.T,
        grad_down,
    )


def solution(mesh):
    placed = (
        P(("dp", "tensor"), None),
        P(("dp", "tensor"), None),
        P(),
        P(None, "tensor"),
        P(None, "tensor"),
        P("tensor", None),
        P(),
        P(None, "tensor"),
        P(None, "tensor"),
        P("tensor", None),
    )
    return jax.shard_map(
        local,
        mesh=mesh,
        in_specs=placed,
        out_specs=(
            P(("dp", "tensor")),
            P(("dp", "tensor"), None),
            P(),
            P("dp", "tensor"),
            P("dp", "tensor"),
            P("tensor", "dp"),
        ),
        check_vma=False,
    )
```

```python
import functools
import math

import jax
import jax.numpy as jnp
from jax import lax
from jax.experimental import pallas as pl
from jax.experimental.pallas import tpu as pltpu
from jax.sharding import PartitionSpec as P

F32 = jnp.float32
BF16 = jnp.bfloat16
MESH = pl.DeviceIdType.MESH
VMEM_LIMIT = 66_000_000
ROWS = 16


def digits(*order):
    return sum(p * 8**k for k, p in enumerate(order))


ARRIVAL = digits(0, 3, 1, 4, 2, 7, 6, 5)
LATE = digits(6, 2, 5, 7, 1, 3, 4, 0)
TERMS = digits(2, 6, 5, 3, 1, 7, 0, 4)
DOWN = digits(2, 1, 3, 0, 6, 5, 7, 4)
ALL, A, B, A0, A1, B0, B1 = (0, 4), (0, 2), (2, 4), (0, 1), (1, 2), (2, 3), (3, 4)


class Wires:
    def __init__(self, send_sems, recv_sems):
        self.send_sems, self.recv_sems, self.sent = send_sems, recv_sems, []

    def send(self, src, dst, out, into, device):
        copy = pltpu.make_async_remote_copy(
            src_ref=src,
            dst_ref=dst,
            send_sem=self.send_sems.at[out],
            recv_sem=self.recv_sems.at[into],
            device_id=device,
            device_id_type=MESH,
        )
        copy.start()
        self.sent.append(copy)

    def got(self, ref, into, device):
        pltpu.make_async_remote_copy(
            src_ref=ref,
            dst_ref=ref,
            send_sem=self.send_sems.at[0],
            recv_sem=self.recv_sems.at[into],
            device_id=device,
            device_id_type=MESH,
        ).wait_recv()

    def drain(self):
        for copy in self.sent:
            copy.wait_send()


class Seat:
    def __init__(self):
        t = lax.axis_index("tensor")
        self.t = t
        self.z, self.y, self.c = t // 4, (t // 2) % 2, t % 2
        self.zp, self.zm, self.zf = (self.z + 1) % 4, (self.z + 3) % 4, (self.z + 2) % 4
        self.o, self.s = 1 - self.y, 1 - self.c

    def dev(self, z, y, c):
        return {"tensor": z * 4 + y * 2 + c}

    def pairs_of(self, code):
        first, second = code % 8, (code // 8) % 8
        return tuple(
            ((self.z + p % 4) % 4) * 2 + (self.y + p // 4) % 2 for p in (first, second)
        )

    def pairs(self, i, order):
        return self.pairs_of(order // 64**i)


def meet(devices):
    barrier = pltpu.get_barrier_semaphore()
    for device in devices:
        pl.semaphore_signal(barrier, inc=1, device_id=device, device_id_type=MESH)
    pl.semaphore_wait(barrier, len(devices))


class Gather:
    def __init__(self, seat, own, full, send_sems, recv_sems):
        self.s, self.own, self.full = seat, own, full
        self.w = Wires(send_sems, recv_sems)
        self.quarter = own.shape[0] // 4

    def rows(self, part):
        return pl.ds(part[0] * self.quarter, (part[1] - part[0]) * self.quarter)

    def blk(self, z, y, c, part):
        return self.full.at[z * 2 + y, c, self.rows(part)]

    def own_to(self, part, out, into, device):
        s = self.s
        self.w.send(self.own.at[self.rows(part)], self.blk(s.z, s.y, s.c, part), out, into, device)

    def pass_on(self, z, y, part, out, into, device):
        b = self.blk(z, y, self.s.c, part)
        self.w.send(b, b, out, into, device)

    def got(self, z, y, part, into):
        s = self.s
        self.w.got(self.blk(z, y, s.c, part), into, s.dev(s.z, s.y, s.s))

    def start(self):
        s = self.s
        up, down, across = s.dev(s.zp, s.y, s.c), s.dev(s.zm, s.y, s.c), s.dev(s.z, s.o, s.c)
        self.own_to(B, 0, 0, up)
        self.own_to(B, 1, 2, down)
        self.own_to(A, 2, 8, across)
        self.own_to(A, 3, 1, up)
        self.own_to(A, 4, 3, down)
        self.own_to(B, 5, 9, across)
        self.own_to(ALL, 6, 17, s.dev(s.z, s.y, s.s))
        self.full[s.z * 2 + s.y, s.c] = self.own[...]

    def arrive(self, *events):
        s = self.s
        z, zp, zm, zf, y, o = s.z, s.zp, s.zm, s.zf, s.y, s.o
        up, down, across = s.dev(zp, y, s.c), s.dev(zm, y, s.c), s.dev(z, o, s.c)
        sib = s.dev(z, y, s.s)
        for e in events:
            if e == 0:
                self.got(zm, y, B, 0)
                self.pass_on(zm, y, B0, 7, 4, up)
                self.pass_on(zm, y, B, 9, 11, across)
                self.got(zp, y, B, 2)
                self.pass_on(zp, y, B1, 8, 5, down)
                self.pass_on(zp, y, B, 10, 13, across)
            if e == 1:
                self.got(z, o, A, 8)
                self.pass_on(z, o, A, 12, 10, up)
                self.pass_on(z, o, A, 13, 12, down)
            if e == 2:
                self.got(zm, y, A, 1)
                self.pass_on(zm, y, A0, 14, 6, up)
                self.pass_on(zm, y, ALL, 18, 18, sib)
                self.got(zp, y, A, 3)
                self.pass_on(zp, y, A1, 15, 7, down)
                self.pass_on(zp, y, ALL, 19, 19, sib)
            if e == 3:
                self.got(z, o, B, 9)
                self.pass_on(z, o, ALL, 21, 21, sib)
            if e == 4:
                self.got(zf, y, B0, 4)
                self.got(zf, y, B1, 5)
                self.pass_on(zf, y, B, 11, 16, across)
            if e == 5:
                self.got(zm, o, A, 10)
                self.pass_on(zm, o, A0, 16, 14, up)
                self.got(zp, o, A, 12)
                self.pass_on(zp, o, A1, 17, 15, down)
            if e == 6:
                self.got(zf, y, A0, 6)
                self.got(zf, y, A1, 7)
                self.pass_on(zf, y, ALL, 20, 20, sib)
            if e == 7:
                self.got(zm, o, B, 11)
                self.pass_on(zm, o, ALL, 22, 22, sib)
                self.got(zp, o, B, 13)
                self.pass_on(zp, o, ALL, 23, 23, sib)
            if e == 8:
                self.got(zf, o, A0, 14)
                self.got(zf, o, A1, 15)
                self.got(zf, o, B, 16)
                self.pass_on(zf, o, ALL, 24, 24, sib)

    def have(self, i):
        s = self.s
        sib = s.dev(s.z, s.y, s.s)
        for p, k in zip(s.pairs(i, ARRIVAL), ((17, 18), (19, 21), (20, 22), (24, 23))[i]):
            self.w.got(self.full.at[p, s.s], k, sib)


def fold(dst, refs):
    def rows(k, carry):
        at = pl.ds(pl.multiple_of(k * ROWS, ROWS), ROWS)
        dst[at] = total_of(refs, at).astype(dst.dtype)
        return carry

    lax.fori_loop(0, dst.shape[0] // ROWS, rows, 0)


class RingFirst:
    def __init__(self, block, dev, ring, row, slots, last, send_sems, recv_sems, base):
        self.block, self.dev, self.slots, self.last, self.base = block, dev, slots, last, base
        self.r, self.y, self.o = ring, row, 1 - row
        self.rp, self.rm, self.rf = (ring + 1) % 4, (ring + 3) % 4, (ring + 2) % 4
        self.w = Wires(send_sems, recv_sems)

    def out(self, r, y, slot, to, more=()):
        refs = self.block(r, y)
        if len(refs) + len(more) > 1:
            fold(refs[0], refs + [self.slots.at[k] for k in more])
        self.w.send(refs[0], self.slots.at[slot], self.base + slot, self.base + slot, to)

    def got(self, slot):
        self.w.got(self.slots.at[slot], self.base + slot, self.dev(self.rp, self.y))

    def ready(self, off, rel):
        up, down = self.dev(self.rp, self.y), self.dev(self.rm, self.y)
        if (off, rel) == (2, 1):
            self.out(self.rf, self.o, 0, up)
        if (off, rel) == (2, 0):
            self.out(self.rf, self.y, 1, down)
        if (off, rel) == (1, 0):
            self.out(self.rp, self.y, 3, up)
        if (off, rel) == (3, 1):
            self.out(self.rm, self.o, 4, down)

    def stage2(self):
        self.got(0)
        self.out(self.rp, self.o, 2, self.dev(self.rp, self.y), (0,))
        self.got(1)
        self.out(self.rm, self.y, 5, self.dev(self.rm, self.y), (1,))

    def stage3(self):
        self.got(4)
        self.got(2)
        refs = self.block(self.r, self.o)
        fold(refs[0], refs + [self.slots.at[2], self.slots.at[4]])
        self.w.send(refs[0], self.last, self.base + 6, self.base + 6, self.dev(self.r, self.o))

    def stage4(self):
        self.got(3)
        self.got(5)
        self.w.got(self.last, self.base + 6, self.dev(self.r, self.o))
        return self.block(self.r, self.y) + [self.slots.at[3], self.slots.at[5], self.last]


class RowFirst:
    def __init__(self, block, dev, ring, row, across, far, near, send_sems, recv_sems, base):
        self.block, self.dev, self.base = block, dev, base
        self.across, self.far, self.near = across, far, near
        self.r, self.y, self.o = ring, row, 1 - row
        self.rp, self.rm, self.rf = (ring + 1) % 4, (ring + 3) % 4, (ring + 2) % 4
        self.up, self.down, self.over = dev(self.rp, row), dev(self.rm, row), dev(ring, self.o)
        self.half = near.shape[1] // 2
        self.w = Wires(send_sems, recv_sems)

    def piece(self, ref, h):
        return ref.at[pl.ds(h * self.half, self.half)]

    def send(self, src, dst, k, to):
        self.w.send(src, dst, self.base + k, self.base + k, to)

    def got(self, ref, k):
        self.w.got(ref, self.base + k, self.over)

    def ready(self, off, rel):
        if rel == 1:
            r = (self.r + off) % 4
            refs = self.block(r, self.o)
            if len(refs) > 1:
                fold(refs[0], refs)
            self.send(refs[0], self.across.at[r], off, self.over)

    def joined(self, r, k):
        self.got(self.across.at[r], k)
        refs = self.block(r, self.y)
        fold(refs[0], refs + [self.across.at[r]])
        return refs[0]

    def far_out(self):
        ref = self.joined(self.rf, 2)
        self.send(self.piece(ref, 0), self.far.at[0], 4, self.up)
        self.send(self.piece(ref, 1), self.far.at[1], 5, self.down)

    def near_out(self):
        ref = self.joined(self.rp, 1)
        self.send(self.piece(ref, 1), self.piece(self.near.at[0], 1), 6, self.up)
        ref = self.joined(self.rm, 3)
        self.send(self.piece(ref, 0), self.piece(self.near.at[1], 0), 7, self.down)

    def stage3(self):
        self.got(self.far.at[0], 4)
        ref = self.piece(self.block(self.rp, self.y)[0], 0)
        fold(ref, [ref, self.far.at[0]])
        self.send(ref, self.piece(self.near.at[0], 0), 8, self.up)
        self.got(self.far.at[1], 5)
        ref = self.piece(self.block(self.rm, self.y)[0], 1)
        fold(ref, [ref, self.far.at[1]])
        self.send(ref, self.piece(self.near.at[1], 1), 9, self.down)

    def stage4(self):
        self.got(self.across.at[self.r], 0)
        for k, h, at in ((0, 1, 6), (1, 0, 7), (0, 0, 8), (1, 1, 9)):
            self.got(self.piece(self.near.at[k], h), at)
        return self.block(self.r, self.y) + [self.across.at[self.r], self.near.at[0], self.near.at[1]]


class GroupSum:
    def __init__(self, seat, order, partial, paired, ring_a, row_a, ring_b, send_sems, recv_sems):
        self.s, self.order, self.partial, self.paired = seat, order, partial, paired
        self.w = Wires(send_sems, recv_sems)
        half = paired.shape[1] // 2

        def block(h):
            at = pl.ds(h * half, half)
            return lambda z, y: [partial.at[z * 2 + y, seat.c, at], paired.at[z * 2 + y, at]]

        def dev(z, y):
            return seat.dev(z, y, seat.c)

        form, buffers = (RowFirst, row_a) if ring_a is None else (RingFirst, ring_a)
        self.a = form(block(0), dev, seat.z, seat.y, *buffers, send_sems, recv_sems, 15)
        self.b = RingFirst(block(1), dev, seat.z, seat.y, *ring_b, send_sems, recv_sems, 8)

    def pair_send(self, i):
        s = self.s
        for j, p in enumerate(s.pairs(i, self.order)):
            k = 2 * i + j
            self.w.send(self.partial.at[p, s.s], self.paired.at[p], k, k, s.dev(s.z, s.y, s.s))

    def ready(self, i):
        s = self.s
        for j, p in enumerate(s.pairs(i, self.order)):
            self.w.got(self.paired.at[p], 2 * i + j, s.dev(s.z, s.y, s.s))
        for j in range(2):
            place = self.order // 8 ** (2 * i + j) % 8
            self.b.ready(place % 4, place // 4)
            self.a.ready(place % 4, place // 4)

    def drain(self):
        for w in (self.w, self.a.w, self.b.w):
            w.drain()


def total_of(refs, at):
    total = refs[0][at].astype(F32)
    for ref in refs[1:]:
        total = total + ref[at].astype(F32)
    return total


def sigmoid(v):
    return 1.0 / (1.0 + jnp.exp(-v))


def dot(a, b):
    return jnp.dot(a, b, preferred_element_type=F32)


def dot_t(a, b):
    return lax.dot_general(a, b, (((1,), (1,)), ((), ())), preferred_element_type=F32)


def tile(j, size):
    return pl.ds(pl.multiple_of(j * size, size), size)


def rows_of(ref, p1, p2, at=slice(None)):
    parts = [ref[p, ..., at] for p in (p1, p2)]
    return jnp.concatenate([v.reshape(-1, v.shape[-1]) for v in parts], axis=0)


def kernel(
    tokens, targets, lgain, fgain, wg, wu, wd, fg, fu, fd,
    scores, grad_tokens, grad_gain, out_gate, out_up, out_down,
    full, normed, fnormed, gate, up, hid_t, hid, lpart, fpart,
    lpaired, fpaired, lslots, fslots, llast, flast, lacross, facross, lfar, ffar, lnear, fnear,
    vwg, vwu, vwd, terms, ograd, flat_scores,
    gg, ug, ggt, ugt, gslots, glast, uslots, ulast, dslots, dfar, dlast, gain_acc, gain_t, gain_d,
    o_scores, o_tokens, o_gain, o_gate, o_up, o_down,
    load_sems, out_sems, gsend, grecv, lsend, lrecv, fsend, frecv,
    qsend, qrecv, dsend, drecv, tsend, trecv, psend, precv,
):
    seat = Seat()
    s = seat
    d = lax.axis_index("dp")
    x, yl = d % 4, d // 4
    block, width = tokens.shape
    hidden, cut = vwg.shape[1], terms.shape[3]
    deep, wide = width // hidden, hidden // cut
    n = 2 * block
    wt = 2 * cut
    moves = []
    for q, src in ((0, fg), (1, fu)):
        for j in range(wide):
            for k in range(deep):
                part = src.at[pl.ds(k * hidden, hidden), pl.ds(j * cut, cut)]
                moves.append((part, terms.at[q, j * deep + k], q))
    moves += [(fd.at[:, pl.ds(k * cut, cut)], terms.at[2, k], 2) for k in range(8)]
    moves += [(wg, vwg, 3), (wu, vwu, 4), (wd, vwd, 5)]

    def loaded(ref, k):
        pltpu.make_async_copy(ref, ref, load_sems.at[k]).wait()

    peers = [{"tensor": (s.t + r) % 16} for r in range(1, 16)]
    peers += [{"dp": (d + r) % 8} for r in range(1, 8)]
    meet(peers)
    gather = Gather(s, tokens, full, gsend, grecv)
    gather.start()
    for src, dst, k in moves:
        pltpu.make_async_copy(src, dst, load_sems.at[k]).start()
    ring_l, ring_f = (lslots, llast), (fslots, flast)
    row_l, row_f = (lacross, lfar, lnear), (facross, ffar, fnear)
    learner = GroupSum(s, LATE, lpart, lpaired, None, row_l, ring_l, lsend, lrecv)
    frozen = GroupSum(s, ARRIVAL, fpart, fpaired, None, row_f, ring_f, fsend, frecv)

    def unit(ref, at):
        v = ref[at].astype(F32)
        return v * lax.rsqrt(jnp.mean(v * v, axis=-1, keepdims=True) + 1e-05)

    def normalize(src, dst, gain):
        def rows(k, carry):
            for h in range(2):
                at = pl.ds(pl.multiple_of(k * 2 * ROWS + h * ROWS, ROWS), ROWS)
                dst[at] = (unit(src, at) * gain[...]).astype(BF16)
            return carry

        lax.fori_loop(0, block // (2 * ROWS), rows, 0)

    def frozen_units(i):
        for j, p in enumerate(s.pairs(i, ARRIVAL)):
            for core in range(2):
                normalize(full.at[p, core], fnormed.at[j, core], fgain)

    def put(part, p1, p2, cols, value):
        value = value.astype(BF16).reshape(2, 2, block, value.shape[-1])
        part[p1, :, :, cols] = value[0]
        part[p2, :, :, cols] = value[1]

    def frozen_hidden():
        def cols(j, carry):
            lhs = rows_of(fnormed, 0, 1)
            at = pl.ds(j * deep, deep)
            g = dot(lhs, terms[0, at].reshape(width, cut))
            u = dot(lhs, terms[1, at].reshape(width, cut))
            hid[:, tile(j, cut)] = (g * sigmoid(g) * u).astype(BF16)
            return carry

        lax.fori_loop(0, wide, cols, 0)

    def frozen_out(i):
        p1, p2 = s.pairs(i, ARRIVAL)

        def outs(j, carry):
            lhs = hid[...]
            value = jnp.concatenate([dot(lhs, terms[2, 2 * j + k]) for k in range(2)], axis=1)
            put(fpart, p1, p2, tile(j, wt), value)
            return carry

        lax.fori_loop(0, 4, outs, 0)

    def learner_units(i):
        for p in s.pairs(i, LATE):
            for core in range(2):
                normalize(full.at[p, core], normed.at[p, core], lgain)

    def learner_hidden(i):
        p1, p2 = s.pairs(i, LATE)

        def cols(j, carry):
            at = tile(j, cut)
            lhs = rows_of(normed, p1, p2)
            g, u = dot(lhs, vwg[:, at]), dot(lhs, vwu[:, at])
            gate[p1, :, at], gate[p2, :, at] = g[:n], g[n:]
            up[p1, :, at], up[p2, :, at] = u[:n], u[n:]
            h = g * sigmoid(g) * u
            hid[:, at] = h.astype(BF16)
            ht = h.T.astype(BF16)
            hid_t[at, tile(p1, n)] = ht[:, :n]
            hid_t[at, tile(p2, n)] = ht[:, n:]
            return carry

        lax.fori_loop(0, wide, cols, 0)

    def learner_out(i):
        p1, p2 = s.pairs(i, LATE)

        def outs(j, carry):
            at = tile(j, wt)
            put(lpart, p1, p2, at, dot(hid[...], vwd[:, at]))
            return carry

        lax.fori_loop(0, width // wt, outs, 0)
        learner.pair_send(i)

    arrivals = (((0, 1, 2), (3, 4), (5,)), ((), (6,), (7,)), ((8,), (), ()), ((), (), ()))
    for i in range(4):
        gather.arrive(*arrivals[i][0])
        gather.have(i)
        frozen_units(i)
        gather.arrive(*arrivals[i][1])
        if i == 0:
            for q in range(3):
                loaded(terms.at[q], q)
        if i > 0:
            frozen.ready(i - 1)
        frozen_hidden()
        gather.arrive(*arrivals[i][2])
        frozen_out(i)
        frozen.pair_send(i)
    learner_units(0)
    frozen.ready(3)
    gather.w.drain()
    for k, ref in ((3, vwg), (4, vwu), (5, vwd)):
        loaded(ref, k)
    learner_hidden(0)
    learner_out(0)
    learner_units(1)
    learner.ready(0)
    learner_hidden(1)
    frozen.b.stage2()
    frozen.a.far_out()
    learner_out(1)
    learner_units(2)
    frozen.a.near_out()
    learner.ready(1)
    learner_hidden(2)
    learner_out(2)
    learner_units(3)
    learner.ready(2)
    frozen.b.stage3()
    learner_hidden(3)
    frozen.a.stage3()
    learner.b.stage2()
    learner_out(3)
    learner.a.far_out()
    learner.a.near_out()
    learner.ready(3)
    learner.b.stage3()
    learner.a.stage3()
    root = math.sqrt(width)

    def losses(frefs, lrefs, base):
        def rows(k, carry):
            at = pl.ds(pl.multiple_of(k * ROWS, ROWS), ROWS)
            here = pl.ds(pl.multiple_of(base + k * ROWS, ROWS), ROWS)
            goal = targets[here].astype(F32)
            fmiss = total_of(frefs, at) - goal
            frozen_loss = 0.5 * jnp.sum(fmiss * fmiss, axis=-1, keepdims=True) / root
            miss = total_of(lrefs, at) - goal
            learner_loss = 0.5 * jnp.sum(miss * miss, axis=-1, keepdims=True) / root
            score = learner_loss - frozen_loss
            flat_scores[here] = jnp.broadcast_to(score, (ROWS, flat_scores.shape[1]))
            ograd[here] = (sigmoid(score) * miss / root).astype(BF16)
            return carry

        lax.fori_loop(0, block // 2 // ROWS, rows, 0)

    fa, fb = frozen.a.stage4(), frozen.b.stage4()
    la = learner.a.stage4()
    losses(fa, la, 0)
    losses(fb, learner.b.stage4(), block // 2)
    regather = Gather(s, ograd, full, gsend, grecv)
    regather.start()
    outs = []

    def emit(src, dst):
        outs.append(pltpu.make_async_copy(src, dst, out_sems.at[len(outs)]))
        outs[-1].start()

    o_scores[...] = flat_scores[...].T[:1]
    gain_acc[...] = jnp.zeros_like(gain_acc)
    frozen.drain()

    learner.drain()
    summed = GroupSum(s, LATE, fpart, fpaired, ring_l, None, ring_f, fsend, frecv)

    def dp_dev(xx, yy):
        return {"dp": yy * 4 + xx}

    def dp_block(q):
        return lambda xx, yy: [terms.at[q, yy * 4 + xx]]

    gate_sum = RingFirst(dp_block(0), dp_dev, x, yl, gslots, glast, qsend, qrecv, 0)
    up_sum = RingFirst(dp_block(1), dp_dev, x, yl, uslots, ulast, qsend, qrecv, 7)
    down_sum = RowFirst(dp_block(2), dp_dev, x, yl, dslots, dfar, dlast, dsend, drecv, 0)

    def back(i):
        p1, p2 = s.pairs(i, ARRIVAL)

        def cols(j, carry):
            at = tile(j, cut)
            hg = dot_t(rows_of(full, p1, p2), vwd[at, :])
            g, u = rows_of(gate, p1, p2, at), rows_of(up, p1, p2, at)
            sigma = sigmoid(g)
            side = hg * sigma
            ggrad = side * u * (1.0 + g * (1.0 - sigma))
            ugrad = side * g
            for value, plain, flipped in ((ggrad, gg, ggt), (ugrad, ug, ugt)):
                low = value.astype(BF16)
                plain[p1, :, at], plain[p2, :, at] = low[:n], low[n:]
                turned = value.T.astype(BF16)
                flipped[at, tile(p1, n)] = turned[:, :n]
                flipped[at, tile(p2, n)] = turned[:, n:]
            return carry

        lax.fori_loop(0, wide, cols, 0)

    for i, events in enumerate(((0, 1, 2, 3), (4, 5), (6, 7), (8,))):
        regather.arrive(*events)
        regather.have(i)
        back(i)

    def term(q, lhs, rhs, dd):
        at = tile(dd, cut)
        terms[q, dd] = dot(lhs[...], rhs[:, :, :, at].reshape(16 * block, cut)).astype(BF16)

    def some_terms(q, lhs, rhs, order, lo, hi):
        def one(k, code):
            row, ring = (yl + 1 + code % 8 // 4) % 2, (x + code % 4) % 4
            term(q, lhs, rhs, row * 4 + ring)
            return code // 8

        lax.fori_loop(lo, hi, one, jnp.int32(order // 8**lo))

    def normed_part(i):
        p1, p2 = s.pairs(i, LATE)

        def outs(j, carry):
            at = tile(j, wt)
            value = dot_t(rows_of(gg, p1, p2), vwg[at, :]) + dot_t(rows_of(ug, p1, p2), vwu[at, :])
            put(fpart, p1, p2, at, value)
            gains = value * rows_of(normed, p1, p2, at).astype(F32)
            gain_acc[:, at] += gains.reshape(-1, 8, wt).sum(axis=0)
            return carry

        lax.fori_loop(0, width // wt, outs, 0)
        summed.pair_send(i)

    def ring_start(q, lhs, ring):
        some_terms(q, lhs, normed, TERMS, 0, 2)
        ring.ready(2, 1)
        ring.ready(2, 0)
        some_terms(q, lhs, normed, TERMS, 2, 4)
        ring.ready(1, 0)
        ring.ready(3, 1)

    ring_start(0, ggt, gate_sum)
    some_terms(2, hid_t, full, DOWN, 0, 4)
    for off in (2, 1, 3, 0):
        down_sum.ready(off, 1)
    ring_start(1, ugt, up_sum)
    normed_part(0)
    normed_part(1)
    summed.ready(0)
    normed_part(2)
    summed.ready(1)
    normed_part(3)
    summed.ready(2)
    gain_t[s.t] = jnp.sum(gain_acc[...], axis=0, keepdims=True) / lgain[...]
    tw, pw = Wires(tsend, trecv), Wires(psend, precv)
    for r in range(1, 16):
        tw.send(gain_t.at[s.t], gain_t.at[s.t], r - 1, r - 1, {"tensor": (s.t + r) % 16})
    some_terms(0, ggt, normed, TERMS, 4, 8)
    gate_sum.stage2()
    summed.ready(3)
    summed.a.stage2()
    summed.b.stage2()
    some_terms(1, ugt, normed, TERMS, 4, 8)
    some_terms(2, hid_t, full, DOWN, 4, 8)
    up_sum.stage2()
    down_sum.far_out()
    down_sum.near_out()
    summed.a.stage3()
    summed.b.stage3()
    for r in range(1, 16):
        tw.got(gain_t.at[(s.t + 16 - r) % 16], r - 1, {"tensor": (s.t + 1) % 16})
    gain_d[d] = jnp.sum(gain_t[...], axis=0)
    for r in range(1, 8):
        pw.send(gain_d.at[d], gain_d.at[d], r - 1, r - 1, {"dp": (d + r) % 8})
    gate_sum.stage3()
    up_sum.stage3()
    down_sum.stage3()

    def token_grads(nrefs, base):
        def rows(k, carry):
            at = pl.ds(pl.multiple_of(k * ROWS, ROWS), ROWS)
            here = pl.ds(pl.multiple_of(base + k * ROWS, ROWS), ROWS)
            v = tokens[here].astype(F32)
            inv = lax.rsqrt(jnp.mean(v * v, axis=-1, keepdims=True) + 1e-05)
            scaled = total_of(nrefs, at) * lgain[...]
            mid = jnp.mean(scaled * v, axis=-1, keepdims=True)
            o_tokens[here] = (inv * scaled - v * (inv * inv * inv * mid)).astype(BF16)
            return carry

        lax.fori_loop(0, block // 2 // ROWS, rows, 0)

    token_grads(summed.a.stage4(), 0)
    token_grads(summed.b.stage4(), block // 2)
    emit(o_tokens, grad_tokens)
    for r in range(1, 8):
        pw.got(gain_d.at[(d + 8 - r) % 8], r - 1, {"dp": (d + 1) % 8})
    o_gain[...] = jnp.sum(gain_d[...], axis=0)
    emit(o_gain, grad_gain)
    emit(o_scores, scores)

    def finish_plain(out, refs):
        def rows(k, carry):
            at = pl.ds(pl.multiple_of(k * ROWS, ROWS), ROWS)
            out[at] = total_of(refs, at)
            return carry

        lax.fori_loop(0, hidden // ROWS, rows, 0)

    def finish_turned(out, refs):
        def rows(k, carry):
            at = tile(k, 128)
            out[:, at] = total_of(refs, at).T
            return carry

        lax.fori_loop(0, hidden // 128, rows, 0)

    finish_turned(o_gate, gate_sum.stage4())
    emit(o_gate, out_gate)
    finish_turned(o_up, up_sum.stage4())
    emit(o_up, out_up)
    finish_plain(o_down, down_sum.stage4())
    emit(o_down, out_down)
    for wires in (summed, regather.w, gate_sum.w, up_sum.w, down_sum.w, tw, pw):
        wires.drain()
    for copy in outs:
        copy.wait()


def hand_over(count, *refs):
    srcs, dsts, held, sems = refs[:count], refs[count : 2 * count], refs[2 * count : -1], refs[-1]
    ins = [pltpu.make_async_copy(a, b, sems.at[0, k]) for k, (a, b) in enumerate(zip(srcs, held))]
    outs = [pltpu.make_async_copy(a, b, sems.at[1, k]) for k, (a, b) in enumerate(zip(held, dsts))]
    for copy in ins:
        copy.start()
    for copy, then in zip(ins, outs):
        copy.wait()
        then.start()
    for copy in outs:
        copy.wait()


def local(
    tokens, targets, learner_gain, learner_gate, learner_up, learner_down,
    frozen_gain, frozen_gate, frozen_up, frozen_down,
):
    block, width = tokens.shape
    hidden = learner_gate.shape[1]
    cut, group, half = width // 8, 16 * block, block // 2
    here = pl.BlockSpec(memory_space=pltpu.VMEM)
    away = pl.BlockSpec(memory_space=pl.ANY)
    shape, vmem = jax.ShapeDtypeStruct, pltpu.VMEM

    def dma(*counts):
        return [pltpu.SemaphoreType.DMA((k,)) for k in counts]

    def twice(*shapes):
        return [vmem((*lead, width), BF16) for lead in shapes for _ in range(2)]

    blocks = vmem((8, 2, block, width), BF16)
    pre = vmem((8, 2 * block, hidden), F32)
    flat = vmem((8, 2 * block, hidden), BF16)
    turned = vmem((hidden, group), BF16)
    ring, mine = vmem((6, hidden, cut), BF16), vmem((hidden, cut), BF16)
    shapes = (
        shape((1, block), F32),
        shape((block, width), BF16),
        shape((1, width), F32),
        shape((cut, hidden), F32),
        shape((cut, hidden), F32),
        shape((hidden, cut), F32),
    )
    held = [vmem(a.shape, a.dtype) for a in shapes]
    results = pl.pallas_call(
        kernel,
        out_shape=shapes,
        in_specs=[here] * 4 + [away] * 6,
        out_specs=[away] * 6,
        scratch_shapes=[blocks, blocks, vmem((2, 2, block, width), BF16), pre, pre, turned]
        + [vmem((4 * block, hidden), BF16), blocks, blocks]
        + twice((8, block), (6, half), (half,), (4, half), (2, half // 2), (2, half))
        + [vmem((width, hidden), BF16)] * 2
        + [vmem((hidden, width), BF16), vmem((3, 8, hidden, cut), BF16)]
        + [vmem((block, width), BF16), vmem((block, 128), F32), flat, flat, turned, turned]
        + [ring, mine, ring, mine]
        + [vmem((k, hidden // h, cut), BF16) for k, h in ((4, 1), (2, 2), (2, 1))]
        + [vmem((8, width), F32), vmem((16, 1, width), F32), vmem((8, 1, width), F32)]
        + held
        + dma(6, 6, 25, 25, 25, 25, 25, 25, 14, 14, 10, 10, 15, 15, 7, 7),
        compiler_params=pltpu.CompilerParams(
            has_side_effects=True, vmem_limit_bytes=VMEM_LIMIT, collective_id=1
        ),
        name="step",
    )(
        tokens, targets, learner_gain.reshape(1, width), frozen_gain.reshape(1, width),
        learner_gate, learner_up, learner_down, frozen_gate, frozen_up, frozen_down,
    )
    scores, grad_tokens, grad_gain, grad_gate, grad_up, grad_down = pl.pallas_call(
        functools.partial(hand_over, len(shapes)),
        out_shape=shapes,
        in_specs=[away] * 6,
        out_specs=[away] * 6,
        scratch_shapes=held + [pltpu.SemaphoreType.DMA((2, 6))],
        name="hand_over",
    )(*results)
    return (
        scores.reshape(block),
        grad_tokens,
        grad_gain.reshape(width),
        grad_gate,
        grad_up,
        grad_down,
    )


def solution(mesh):
    placed = (
        P(("dp", "tensor"), None),
        P(("dp", "tensor"), None),
        P(),
        P(None, "tensor"),
        P(None, "tensor"),
        P("tensor", None),
        P(),
        P(None, "tensor"),
        P(None, "tensor"),
        P("tensor", None),
    )
    return jax.shard_map(
        local,
        mesh=mesh,
        in_specs=placed,
        out_specs=(
            P(("dp", "tensor")),
            P(("dp", "tensor"), None),
            P(),
            P("dp", "tensor"),
            P("dp", "tensor"),
            P("tensor", "dp"),
        ),
        check_vma=False,
    )
```

```python
import functools
import math

import jax
import jax.numpy as jnp
from jax import lax
from jax.experimental import pallas as pl
from jax.experimental.pallas import tpu as pltpu
from jax.sharding import PartitionSpec as P

F32 = jnp.float32
BF16 = jnp.bfloat16
MESH = pl.DeviceIdType.MESH
VMEM_LIMIT = 66_000_000
ROWS = 16


def digits(*order):
    return sum(p * 8**k for k, p in enumerate(order))


ARRIVAL = digits(0, 3, 1, 4, 2, 7, 6, 5)
LATE = digits(6, 2, 5, 3, 7, 4, 1, 0)
TERMS = digits(2, 6, 5, 3, 1, 7, 0, 4)
DOWN = digits(2, 1, 3, 0, 6, 5, 7, 4)
ALL, A, B, A0, A1, B0, B1 = (0, 4), (0, 2), (2, 4), (0, 1), (1, 2), (2, 3), (3, 4)


class Wires:
    def __init__(self, send_sems, recv_sems):
        self.send_sems, self.recv_sems, self.sent = send_sems, recv_sems, []

    def send(self, src, dst, out, into, device):
        copy = pltpu.make_async_remote_copy(
            src_ref=src,
            dst_ref=dst,
            send_sem=self.send_sems.at[out],
            recv_sem=self.recv_sems.at[into],
            device_id=device,
            device_id_type=MESH,
        )
        copy.start()
        self.sent.append(copy)

    def got(self, ref, into, device):
        pltpu.make_async_remote_copy(
            src_ref=ref,
            dst_ref=ref,
            send_sem=self.send_sems.at[0],
            recv_sem=self.recv_sems.at[into],
            device_id=device,
            device_id_type=MESH,
        ).wait_recv()

    def drain(self):
        for copy in self.sent:
            copy.wait_send()


class Seat:
    def __init__(self):
        t = lax.axis_index("tensor")
        self.t = t
        self.z, self.y, self.c = t // 4, (t // 2) % 2, t % 2
        self.zp, self.zm, self.zf = (self.z + 1) % 4, (self.z + 3) % 4, (self.z + 2) % 4
        self.o, self.s = 1 - self.y, 1 - self.c

    def dev(self, z, y, c):
        return {"tensor": z * 4 + y * 2 + c}

    def pairs_of(self, code):
        first, second = code % 8, (code // 8) % 8
        return tuple(
            ((self.z + p % 4) % 4) * 2 + (self.y + p // 4) % 2 for p in (first, second)
        )

    def pairs(self, i, order):
        return self.pairs_of(order // 64**i)


def meet(devices):
    barrier = pltpu.get_barrier_semaphore()
    for device in devices:
        pl.semaphore_signal(barrier, inc=1, device_id=device, device_id_type=MESH)
    pl.semaphore_wait(barrier, len(devices))


class Gather:
    def __init__(self, seat, own, full, send_sems, recv_sems):
        self.s, self.own, self.full = seat, own, full
        self.w = Wires(send_sems, recv_sems)
        self.quarter = own.shape[0] // 4

    def rows(self, part):
        return pl.ds(part[0] * self.quarter, (part[1] - part[0]) * self.quarter)

    def blk(self, z, y, c, part):
        return self.full.at[z * 2 + y, c, self.rows(part)]

    def own_to(self, part, out, into, device):
        s = self.s
        self.w.send(self.own.at[self.rows(part)], self.blk(s.z, s.y, s.c, part), out, into, device)

    def pass_on(self, z, y, part, out, into, device):
        b = self.blk(z, y, self.s.c, part)
        self.w.send(b, b, out, into, device)

    def got(self, z, y, part, into):
        s = self.s
        self.w.got(self.blk(z, y, s.c, part), into, s.dev(s.z, s.y, s.s))

    def start(self):
        s = self.s
        up, down, across = s.dev(s.zp, s.y, s.c), s.dev(s.zm, s.y, s.c), s.dev(s.z, s.o, s.c)
        self.own_to(B, 0, 0, up)
        self.own_to(B, 1, 2, down)
        self.own_to(A, 2, 8, across)
        self.own_to(A, 3, 1, up)
        self.own_to(A, 4, 3, down)
        self.own_to(B, 5, 9, across)
        self.own_to(ALL, 6, 17, s.dev(s.z, s.y, s.s))
        self.full[s.z * 2 + s.y, s.c] = self.own[...]

    def arrive(self, *events):
        s = self.s
        z, zp, zm, zf, y, o = s.z, s.zp, s.zm, s.zf, s.y, s.o
        up, down, across = s.dev(zp, y, s.c), s.dev(zm, y, s.c), s.dev(z, o, s.c)
        sib = s.dev(z, y, s.s)
        for e in events:
            if e == 0:
                self.got(zm, y, B, 0)
                self.pass_on(zm, y, B0, 7, 4, up)
                self.pass_on(zm, y, B, 9, 11, across)
                self.got(zp, y, B, 2)
                self.pass_on(zp, y, B1, 8, 5, down)
                self.pass_on(zp, y, B, 10, 13, across)
            if e == 1:
                self.got(z, o, A, 8)
                self.pass_on(z, o, A, 12, 10, up)
                self.pass_on(z, o, A, 13, 12, down)
            if e == 2:
                self.got(zm, y, A, 1)
                self.pass_on(zm, y, A0, 14, 6, up)
                self.pass_on(zm, y, ALL, 18, 18, sib)
                self.got(zp, y, A, 3)
                self.pass_on(zp, y, A1, 15, 7, down)
                self.pass_on(zp, y, ALL, 19, 19, sib)
            if e == 3:
                self.got(z, o, B, 9)
                self.pass_on(z, o, ALL, 21, 21, sib)
            if e == 4:
                self.got(zf, y, B0, 4)
                self.got(zf, y, B1, 5)
                self.pass_on(zf, y, B, 11, 16, across)
            if e == 5:
                self.got(zm, o, A, 10)
                self.pass_on(zm, o, A0, 16, 14, up)
                self.got(zp, o, A, 12)
                self.pass_on(zp, o, A1, 17, 15, down)
            if e == 6:
                self.got(zf, y, A0, 6)
                self.got(zf, y, A1, 7)
                self.pass_on(zf, y, ALL, 20, 20, sib)
            if e == 7:
                self.got(zm, o, B, 11)
                self.pass_on(zm, o, ALL, 22, 22, sib)
                self.got(zp, o, B, 13)
                self.pass_on(zp, o, ALL, 23, 23, sib)
            if e == 8:
                self.got(zf, o, A0, 14)
                self.got(zf, o, A1, 15)
                self.got(zf, o, B, 16)
                self.pass_on(zf, o, ALL, 24, 24, sib)

    def have(self, i):
        s = self.s
        sib = s.dev(s.z, s.y, s.s)
        for p, k in zip(s.pairs(i, ARRIVAL), ((17, 18), (19, 21), (20, 22), (24, 23))[i]):
            self.w.got(self.full.at[p, s.s], k, sib)


def fold(dst, refs):
    def rows(k, carry):
        at = pl.ds(pl.multiple_of(k * ROWS, ROWS), ROWS)
        dst[at] = total_of(refs, at).astype(dst.dtype)
        return carry

    lax.fori_loop(0, dst.shape[0] // ROWS, rows, 0)


class RingFirst:
    def __init__(self, block, dev, ring, row, slots, last, send_sems, recv_sems, base):
        self.block, self.dev, self.slots, self.last, self.base = block, dev, slots, last, base
        self.r, self.y, self.o = ring, row, 1 - row
        self.rp, self.rm, self.rf = (ring + 1) % 4, (ring + 3) % 4, (ring + 2) % 4
        self.w = Wires(send_sems, recv_sems)

    def out(self, r, y, slot, to, more=()):
        refs = self.block(r, y)
        if len(refs) + len(more) > 1:
            fold(refs[0], refs + [self.slots.at[k] for k in more])
        self.w.send(refs[0], self.slots.at[slot], self.base + slot, self.base + slot, to)

    def got(self, slot):
        self.w.got(self.slots.at[slot], self.base + slot, self.dev(self.rp, self.y))

    def ready(self, off, rel):
        up, down = self.dev(self.rp, self.y), self.dev(self.rm, self.y)
        if (off, rel) == (2, 1):
            self.out(self.rf, self.o, 0, up)
        if (off, rel) == (2, 0):
            self.out(self.rf, self.y, 1, down)
        if (off, rel) == (1, 0):
            self.out(self.rp, self.y, 3, up)
        if (off, rel) == (3, 1):
            self.out(self.rm, self.o, 4, down)

    def stage2(self):
        self.got(0)
        self.out(self.rp, self.o, 2, self.dev(self.rp, self.y), (0,))
        self.got(1)
        self.out(self.rm, self.y, 5, self.dev(self.rm, self.y), (1,))

    def stage3(self):
        self.got(4)
        self.got(2)
        refs = self.block(self.r, self.o)
        fold(refs[0], refs + [self.slots.at[2], self.slots.at[4]])
        self.w.send(refs[0], self.last, self.base + 6, self.base + 6, self.dev(self.r, self.o))

    def stage4(self):
        self.got(3)
        self.got(5)
        self.w.got(self.last, self.base + 6, self.dev(self.r, self.o))
        return self.block(self.r, self.y) + [self.slots.at[3], self.slots.at[5], self.last]


class RowFirst:
    def __init__(self, block, dev, ring, row, across, far, near, send_sems, recv_sems, base):
        self.block, self.dev, self.base = block, dev, base
        self.across, self.far, self.near = across, far, near
        self.r, self.y, self.o = ring, row, 1 - row
        self.rp, self.rm, self.rf = (ring + 1) % 4, (ring + 3) % 4, (ring + 2) % 4
        self.up, self.down, self.over = dev(self.rp, row), dev(self.rm, row), dev(ring, self.o)
        self.half = near.shape[1] // 2
        self.w = Wires(send_sems, recv_sems)

    def piece(self, ref, h):
        return ref.at[pl.ds(h * self.half, self.half)]

    def send(self, src, dst, k, to):
        self.w.send(src, dst, self.base + k, self.base + k, to)

    def got(self, ref, k):
        self.w.got(ref, self.base + k, self.over)

    def ready(self, off, rel):
        if rel == 1:
            r = (self.r + off) % 4
            refs = self.block(r, self.o)
            if len(refs) > 1:
                fold(refs[0], refs)
            self.send(refs[0], self.across.at[r], off, self.over)

    def joined(self, r, k):
        self.got(self.across.at[r], k)
        refs = self.block(r, self.y)
        fold(refs[0], refs + [self.across.at[r]])
        return refs[0]

    def far_out(self):
        ref = self.joined(self.rf, 2)
        self.send(self.piece(ref, 0), self.far.at[0], 4, self.up)
        self.send(self.piece(ref, 1), self.far.at[1], 5, self.down)

    def near_out(self):
        ref = self.joined(self.rp, 1)
        self.send(self.piece(ref, 1), self.piece(self.near.at[0], 1), 6, self.up)
        ref = self.joined(self.rm, 3)
        self.send(self.piece(ref, 0), self.piece(self.near.at[1], 0), 7, self.down)

    def stage3(self):
        self.got(self.far.at[0], 4)
        ref = self.piece(self.block(self.rp, self.y)[0], 0)
        fold(ref, [ref, self.far.at[0]])
        self.send(ref, self.piece(self.near.at[0], 0), 8, self.up)
        self.got(self.far.at[1], 5)
        ref = self.piece(self.block(self.rm, self.y)[0], 1)
        fold(ref, [ref, self.far.at[1]])
        self.send(ref, self.piece(self.near.at[1], 1), 9, self.down)

    def stage4(self):
        self.got(self.across.at[self.r], 0)
        for k, h, at in ((0, 1, 6), (1, 0, 7), (0, 0, 8), (1, 1, 9)):
            self.got(self.piece(self.near.at[k], h), at)
        return self.block(self.r, self.y) + [self.across.at[self.r], self.near.at[0], self.near.at[1]]


class GroupSum:
    def __init__(self, seat, order, partial, paired, ring_a, row_a, ring_b, send_sems, recv_sems):
        self.s, self.order, self.partial, self.paired = seat, order, partial, paired
        self.w = Wires(send_sems, recv_sems)
        half = paired.shape[1] // 2

        def block(h):
            at = pl.ds(h * half, half)
            return lambda z, y: [partial.at[z * 2 + y, seat.c, at], paired.at[z * 2 + y, at]]

        def dev(z, y):
            return seat.dev(z, y, seat.c)

        form, buffers = (RowFirst, row_a) if ring_a is None else (RingFirst, ring_a)
        self.a = form(block(0), dev, seat.z, seat.y, *buffers, send_sems, recv_sems, 15)
        self.b = RingFirst(block(1), dev, seat.z, seat.y, *ring_b, send_sems, recv_sems, 8)

    def pair_send(self, i):
        s = self.s
        for j, p in enumerate(s.pairs(i, self.order)):
            k = 2 * i + j
            self.w.send(self.partial.at[p, s.s], self.paired.at[p], k, k, s.dev(s.z, s.y, s.s))

    def ready(self, i):
        s = self.s
        for j, p in enumerate(s.pairs(i, self.order)):
            self.w.got(self.paired.at[p], 2 * i + j, s.dev(s.z, s.y, s.s))
        for j in range(2):
            place = self.order // 8 ** (2 * i + j) % 8
            self.b.ready(place % 4, place // 4)
            self.a.ready(place % 4, place // 4)

    def drain(self):
        for w in (self.w, self.a.w, self.b.w):
            w.drain()


def total_of(refs, at):
    total = refs[0][at].astype(F32)
    for ref in refs[1:]:
        total = total + ref[at].astype(F32)
    return total


def sigmoid(v):
    return 1.0 / (1.0 + jnp.exp(-v))


def dot(a, b):
    return jnp.dot(a, b, preferred_element_type=F32)


def dot_t(a, b):
    return lax.dot_general(a, b, (((1,), (1,)), ((), ())), preferred_element_type=F32)


def tile(j, size):
    return pl.ds(pl.multiple_of(j * size, size), size)


def rows_of(ref, p1, p2, at=slice(None)):
    parts = [ref[p, ..., at] for p in (p1, p2)]
    return jnp.concatenate([v.reshape(-1, v.shape[-1]) for v in parts], axis=0)


def kernel(
    tokens, targets, lgain, fgain, wg, wu, wd, fg, fu, fd,
    scores, grad_tokens, grad_gain, out_gate, out_up, out_down,
    full, normed, fnormed, gate, up, hid_t, hid, lpart, fpart,
    lpaired, fpaired, lslots, fslots, llast, flast, lacross, facross, lfar, ffar, lnear, fnear,
    again, nslots, nlast, turn_w, row_w, col_w,
    vwg, vwu, vwd, terms, ograd, flat_scores,
    gg, ug, ggt, ugt, gslots, glast, uslots, ulast, dslots, dfar, dlast, gain_acc, gain_t, gain_d,
    o_scores, o_tokens, o_gain, o_gate, o_up, o_down,
    load_sems, out_sems, gsend, grecv, lsend, lrecv, fsend, frecv,
    qsend, qrecv, dsend, drecv, tsend, trecv, psend, precv, wsend, wrecv,
):
    seat = Seat()
    s = seat
    d = lax.axis_index("dp")
    x, yl = d % 4, d // 4
    block, width = tokens.shape
    hidden, cut = vwg.shape[1], terms.shape[3]
    deep, wide = width // hidden, hidden // cut
    n = 2 * block
    wt = 2 * cut
    moves = [(wg, vwg, 3), (wu, vwu, 4), (wd, vwd, 5)]
    for q, src in ((0, fg), (1, fu)):
        for j in range(wide):
            for k in range(deep):
                part = src.at[pl.ds(k * hidden, hidden), pl.ds(j * cut, cut)]
                moves.append((part, terms.at[q, j * deep + k], q))
    moves += [(fd.at[:, pl.ds(k * cut, cut)], terms.at[2, k], 2) for k in range(8)]

    def loaded(ref, k):
        pltpu.make_async_copy(ref, ref, load_sems.at[k]).wait()

    peers = [{"tensor": (s.t + r) % 16} for r in range(1, 16)]
    peers += [{"dp": (d + r) % 8} for r in range(1, 8)]
    meet(peers)
    gather = Gather(s, tokens, full, gsend, grecv)
    gather.start()
    for src, dst, k in moves:
        pltpu.make_async_copy(src, dst, load_sems.at[k]).start()
    ring_l, ring_f = (lslots, llast), (fslots, flast)
    row_l, row_f = (lacross, lfar, lnear), (facross, ffar, fnear)
    learner = GroupSum(s, ARRIVAL, lpart, lpaired, None, row_l, ring_l, lsend, lrecv)
    frozen = GroupSum(s, LATE, fpart, fpaired, None, row_f, ring_f, fsend, frecv)

    def unit(ref, at):
        v = ref[at].astype(F32)
        return v * lax.rsqrt(jnp.mean(v * v, axis=-1, keepdims=True) + 1e-05)

    def normalize(src, dst, gain):
        for k in range(block // ROWS):
            at = pl.ds(k * ROWS, ROWS)
            dst[at] = (unit(src, at) * gain[...]).astype(BF16)

    def frozen_units(i):
        for j, p in enumerate(s.pairs(i, LATE)):

            def one(core, carry, j=j, p=p):
                normalize(full.at[p, core], fnormed.at[j, core], fgain)
                return carry

            lax.fori_loop(0, 2, one, 0)

    def put(part, p1, p2, cols, value):
        value = value.astype(BF16).reshape(2, 2, block, value.shape[-1])
        part[p1, :, :, cols] = value[0]
        part[p2, :, :, cols] = value[1]

    def frozen_hidden():
        def cols(j, carry):
            lhs = rows_of(fnormed, 0, 1)
            at = pl.ds(j * deep, deep)
            g = dot(lhs, terms[0, at].reshape(width, cut))
            u = dot(lhs, terms[1, at].reshape(width, cut))
            hid[:, tile(j, cut)] = (g * sigmoid(g) * u).astype(BF16)
            return carry

        lax.fori_loop(0, wide, cols, 0, unroll=True)

    def frozen_out(i):
        p1, p2 = s.pairs(i, LATE)

        def outs(j, carry):
            lhs = hid[...]
            value = jnp.concatenate([dot(lhs, terms[2, 2 * j + k]) for k in range(2)], axis=1)
            put(fpart, p1, p2, tile(j, wt), value)
            return carry

        lax.fori_loop(0, 4, outs, 0, unroll=True)
        frozen.pair_send(i)

    def learner_units(i):
        for p in s.pairs(i, ARRIVAL):

            def one(core, carry, p=p):
                normalize(full.at[p, core], normed.at[p, core], lgain)
                return carry

            lax.fori_loop(0, 2, one, 0)

    def learner_hidden(i):
        p1, p2 = s.pairs(i, ARRIVAL)

        def cols(j, carry):
            at = tile(j, cut)
            lhs = rows_of(normed, p1, p2)
            g, u = dot(lhs, vwg[:, at]), dot(lhs, vwu[:, at])
            gate[p1, :, at], gate[p2, :, at] = g[:n], g[n:]
            up[p1, :, at], up[p2, :, at] = u[:n], u[n:]
            h = g * sigmoid(g) * u
            hid[:, at] = h.astype(BF16)
            ht = h.T.astype(BF16)
            hid_t[at, tile(p1, n)] = ht[:, :n]
            hid_t[at, tile(p2, n)] = ht[:, n:]
            return carry

        lax.fori_loop(0, wide, cols, 0, unroll=True)

    def learner_out(i):
        p1, p2 = s.pairs(i, ARRIVAL)

        def outs(j, carry):
            at = tile(j, wt)
            put(lpart, p1, p2, at, dot(hid[...], vwd[:, at]))
            return carry

        lax.fori_loop(0, width // wt, outs, 0, unroll=True)
        learner.pair_send(i)

    arrivals = (((0, 1, 2), (3, 4), (5,)), ((), (6,), (7,)), ((8,), (), ()), ((), (), ()))
    for i in range(4):
        gather.arrive(*arrivals[i][0])
        gather.have(i)
        learner_units(i)
        gather.arrive(*arrivals[i][1])
        if i == 0:
            for k, ref in ((3, vwg), (4, vwu), (5, vwd)):
                loaded(ref, k)
        if i > 0:
            learner.ready(i - 1)
        learner_hidden(i)
        gather.arrive(*arrivals[i][2])
        learner_out(i)
    frozen_units(0)
    learner.ready(3)
    gather.w.drain()
    for q in range(3):
        loaded(terms.at[q], q)
    frozen_hidden()
    frozen_out(0)
    frozen_units(1)
    frozen.ready(0)
    frozen_hidden()
    learner.b.stage2()
    frozen_out(1)
    frozen_units(2)
    learner.a.far_out()
    frozen.ready(1)
    frozen_hidden()
    learner.a.near_out()
    frozen_out(2)
    frozen_units(3)
    learner.b.stage3()
    frozen.ready(2)
    learner.a.stage3()
    frozen.b.stage2()
    frozen_hidden()
    frozen.a.far_out()
    frozen_out(3)
    root = math.sqrt(width)

    def misses(refs, base):
        def rows(k, carry):
            at = pl.ds(pl.multiple_of(k * ROWS, ROWS), ROWS)
            here = pl.ds(pl.multiple_of(base + k * ROWS, ROWS), ROWS)
            miss = total_of(refs, at) - targets[here].astype(F32)
            loss = 0.5 * jnp.sum(miss * miss, axis=-1, keepdims=True) / root
            flat_scores[here] = jnp.broadcast_to(loss, (ROWS, flat_scores.shape[1]))
            ograd[here] = (miss / root).astype(BF16)
            return carry

        lax.fori_loop(0, block // 2 // ROWS, rows, 0)

    def weights(refs, base):
        def rows(k, carry):
            at = pl.ds(pl.multiple_of(k * ROWS, ROWS), ROWS)
            here = pl.ds(pl.multiple_of(base + k * ROWS, ROWS), ROWS)
            there = pl.ds(pl.multiple_of(s.c * block + base + k * ROWS, ROWS), ROWS)
            miss = total_of(refs, at) - targets[here].astype(F32)
            loss = 0.5 * jnp.sum(miss * miss, axis=-1, keepdims=True) / root
            score = flat_scores[here] - jnp.broadcast_to(loss, (ROWS, flat_scores.shape[1]))
            flat_scores[here] = score
            turn_w[there] = sigmoid(score)
            return carry

        lax.fori_loop(0, block // 2 // ROWS, rows, 0)

    misses(learner.a.stage4(), 0)
    misses(learner.b.stage4(), block // 2)
    regather = Gather(s, ograd, again, gsend, grecv)
    regather.start()
    frozen.ready(3)
    frozen.a.near_out()
    frozen.b.stage3()
    frozen.a.stage3()
    turn_w[...] = jnp.zeros_like(turn_w)
    outs = []

    def emit(src, dst):
        outs.append(pltpu.make_async_copy(src, dst, out_sems.at[len(outs)]))
        outs[-1].start()

    gain_acc[...] = jnp.zeros_like(gain_acc)

    learner.drain()
    summed = GroupSum(s, LATE, lpart, lpaired, (nslots, nlast), None, ring_l, lsend, lrecv)

    def dp_dev(xx, yy):
        return {"dp": yy * 4 + xx}

    def dp_block(q):
        return lambda xx, yy: [terms.at[q, yy * 4 + xx]]

    gate_sum = RingFirst(dp_block(0), dp_dev, x, yl, gslots, glast, qsend, qrecv, 0)
    up_sum = RingFirst(dp_block(1), dp_dev, x, yl, uslots, ulast, qsend, qrecv, 7)
    down_sum = RowFirst(dp_block(2), dp_dev, x, yl, dslots, dfar, dlast, dsend, drecv, 0)

    def back(i):
        p1, p2 = s.pairs(i, ARRIVAL)

        def cols(j, carry):
            at = tile(j, cut)
            hg = dot_t(rows_of(again, p1, p2), vwd[at, :])
            g, u = rows_of(gate, p1, p2, at), rows_of(up, p1, p2, at)
            sigma = sigmoid(g)
            side = hg * sigma
            ggrad = side * u * (1.0 + g * (1.0 - sigma))
            ugrad = side * g
            for value, plain, flipped in ((ggrad, gg, ggt), (ugrad, ug, ugt)):
                low = value.astype(BF16)
                plain[p1, :, at], plain[p2, :, at] = low[:n], low[n:]
                turned = value.T.astype(BF16)
                flipped[at, tile(p1, n)] = turned[:, :n]
                flipped[at, tile(p2, n)] = turned[:, n:]
            return carry

        lax.fori_loop(0, wide, cols, 0, unroll=True)

    ww = Wires(wsend, wrecv)
    regather.arrive(0, 1, 2)
    regather.have(0)
    back(0)
    regather.arrive(3, 4)
    weights(frozen.a.stage4(), 0)
    weights(frozen.b.stage4(), block // 2)
    row_w[s.t] = turn_w[...].T[:1]
    for r in range(1, 16):
        ww.send(row_w.at[s.t], row_w.at[s.t], r - 1, r - 1, {"tensor": (s.t + r) % 16})
    regather.arrive(5)
    regather.have(1)
    back(1)
    regather.arrive(6, 7)
    regather.have(2)
    back(2)
    regather.arrive(8)
    regather.have(3)
    back(3)
    o_scores[...] = flat_scores[...].T[:1]
    for r in range(1, 16):
        ww.got(row_w.at[(s.t + 16 - r) % 16], r - 1, {"tensor": (s.t + 1) % 16})
    frozen.drain()
    columns = jnp.concatenate([row_w[k] for k in range(16)], axis=0).T
    for p in range(8):
        both = columns[:, 2 * p : 2 * p + 1] + columns[:, 2 * p + 1 : 2 * p + 2]
        col_w[p] = jnp.broadcast_to(both, col_w.shape[1:])

    def weigh(ref):
        for p in range(8):
            at = pl.ds(p * n, n)
            ref[:, at] = (ref[:, at].astype(F32) * (row_w[2 * p] + row_w[2 * p + 1])).astype(BF16)

    def term(q, lhs, rhs, dd):
        at = tile(dd, cut)
        terms[q, dd] = dot(lhs[...], rhs[:, :, :, at].reshape(16 * block, cut)).astype(BF16)

    def some_terms(q, lhs, rhs, order, lo, hi):
        def one(k, code):
            row, ring = (yl + 1 + code % 8 // 4) % 2, (x + code % 4) % 4
            term(q, lhs, rhs, row * 4 + ring)
            return code // 8

        lax.fori_loop(lo, hi, one, jnp.int32(order // 8**lo), unroll=2)

    def normed_part(i):
        p1, p2 = s.pairs(i, LATE)

        def outs(j, carry):
            at = tile(j, wt)
            value = dot_t(rows_of(gg, p1, p2), vwg[at, :]) + dot_t(rows_of(ug, p1, p2), vwu[at, :])
            value = value * jnp.concatenate([col_w[p1, :, :1], col_w[p2, :, :1]], axis=0)
            put(lpart, p1, p2, at, value)
            gains = value * rows_of(normed, p1, p2, at).astype(F32)
            gain_acc[:, at] += gains.reshape(-1, 8, wt).sum(axis=0)
            return carry

        lax.fori_loop(0, width // wt, outs, 0, unroll=True)
        summed.pair_send(i)

    def ring_start(q, lhs, ring):
        some_terms(q, lhs, normed, TERMS, 0, 2)
        ring.ready(2, 1)
        ring.ready(2, 0)
        some_terms(q, lhs, normed, TERMS, 2, 4)
        ring.ready(1, 0)
        ring.ready(3, 1)

    weigh(ggt)
    ring_start(0, ggt, gate_sum)
    weigh(hid_t)
    some_terms(2, hid_t, again, DOWN, 0, 4)
    for off in (2, 1, 3, 0):
        down_sum.ready(off, 1)
    weigh(ugt)
    ring_start(1, ugt, up_sum)
    normed_part(0)
    normed_part(1)
    summed.ready(0)
    normed_part(2)
    summed.ready(1)
    normed_part(3)
    summed.ready(2)
    gain_t[s.t] = jnp.sum(gain_acc[...], axis=0, keepdims=True) / lgain[...]
    tw, pw = Wires(tsend, trecv), Wires(psend, precv)
    for r in range(1, 16):
        tw.send(gain_t.at[s.t], gain_t.at[s.t], r - 1, r - 1, {"tensor": (s.t + r) % 16})
    some_terms(0, ggt, normed, TERMS, 4, 8)
    gate_sum.stage2()
    summed.ready(3)
    summed.a.stage2()
    summed.b.stage2()
    some_terms(1, ugt, normed, TERMS, 4, 8)
    some_terms(2, hid_t, again, DOWN, 4, 8)
    up_sum.stage2()
    down_sum.far_out()
    down_sum.near_out()
    summed.a.stage3()
    summed.b.stage3()
    for r in range(1, 16):
        tw.got(gain_t.at[(s.t + 16 - r) % 16], r - 1, {"tensor": (s.t + 1) % 16})
    gain_d[d] = jnp.sum(gain_t[...], axis=0)
    for r in range(1, 8):
        pw.send(gain_d.at[d], gain_d.at[d], r - 1, r - 1, {"dp": (d + r) % 8})
    gate_sum.stage3()
    up_sum.stage3()
    down_sum.stage3()

    def token_grads(nrefs, base):
        def rows(k, carry):
            at = pl.ds(pl.multiple_of(k * ROWS, ROWS), ROWS)
            here = pl.ds(pl.multiple_of(base + k * ROWS, ROWS), ROWS)
            v = tokens[here].astype(F32)
            inv = lax.rsqrt(jnp.mean(v * v, axis=-1, keepdims=True) + 1e-05)
            scaled = total_of(nrefs, at) * lgain[...]
            mid = jnp.mean(scaled * v, axis=-1, keepdims=True)
            o_tokens[here] = (inv * scaled - v * (inv * inv * inv * mid)).astype(BF16)
            return carry

        lax.fori_loop(0, block // 2 // ROWS, rows, 0)

    token_grads(summed.a.stage4(), 0)
    token_grads(summed.b.stage4(), block // 2)
    emit(o_tokens, grad_tokens)
    for r in range(1, 8):
        pw.got(gain_d.at[(d + 8 - r) % 8], r - 1, {"dp": (d + 1) % 8})
    o_gain[...] = jnp.sum(gain_d[...], axis=0)
    emit(o_gain, grad_gain)
    emit(o_scores, scores)

    def finish_plain(out, refs):
        def rows(k, carry):
            at = pl.ds(pl.multiple_of(k * ROWS, ROWS), ROWS)
            out[at] = total_of(refs, at)
            return carry

        lax.fori_loop(0, hidden // ROWS, rows, 0)

    def finish_turned(out, refs):
        def rows(k, carry):
            at = tile(k, 128)
            out[:, at] = total_of(refs, at).T
            return carry

        lax.fori_loop(0, hidden // 128, rows, 0)

    finish_turned(o_gate, gate_sum.stage4())
    emit(o_gate, out_gate)
    finish_turned(o_up, up_sum.stage4())
    emit(o_up, out_up)
    finish_plain(o_down, down_sum.stage4())
    emit(o_down, out_down)
    for wires in (summed, regather.w, gate_sum.w, up_sum.w, down_sum.w, tw, pw, ww):
        wires.drain()
    for copy in outs:
        copy.wait()


def hand_over(count, *refs):
    srcs, dsts, held, sems = refs[:count], refs[count : 2 * count], refs[2 * count : -1], refs[-1]
    ins = [pltpu.make_async_copy(a, b, sems.at[0, k]) for k, (a, b) in enumerate(zip(srcs, held))]
    outs = [pltpu.make_async_copy(a, b, sems.at[1, k]) for k, (a, b) in enumerate(zip(held, dsts))]
    for copy in ins:
        copy.start()
    for copy, then in zip(ins, outs):
        copy.wait()
        then.start()
    for copy in outs:
        copy.wait()


def local(
    tokens, targets, learner_gain, learner_gate, learner_up, learner_down,
    frozen_gain, frozen_gate, frozen_up, frozen_down,
):
    block, width = tokens.shape
    hidden = learner_gate.shape[1]
    cut, group, half = width // 8, 16 * block, block // 2
    here = pl.BlockSpec(memory_space=pltpu.VMEM)
    away = pl.BlockSpec(memory_space=pl.ANY)
    shape, vmem = jax.ShapeDtypeStruct, pltpu.VMEM

    def dma(*counts):
        return [pltpu.SemaphoreType.DMA((k,)) for k in counts]

    def twice(*shapes):
        return [vmem((*lead, width), BF16) for lead in shapes for _ in range(2)]

    blocks = vmem((8, 2, block, width), BF16)
    pre = vmem((8, 2 * block, hidden), F32)
    flat = vmem((8, 2 * block, hidden), BF16)
    turned = vmem((hidden, group), BF16)
    ring, mine = vmem((6, hidden, cut), BF16), vmem((hidden, cut), BF16)
    shapes = (
        shape((1, block), F32),
        shape((block, width), BF16),
        shape((1, width), F32),
        shape((cut, hidden), F32),
        shape((cut, hidden), F32),
        shape((hidden, cut), F32),
    )
    held = [vmem(a.shape, a.dtype) for a in shapes]
    results = pl.pallas_call(
        kernel,
        out_shape=shapes,
        in_specs=[here] * 4 + [away] * 6,
        out_specs=[away] * 6,
        scratch_shapes=[blocks, blocks, vmem((2, 2, block, width), BF16), pre, pre, turned]
        + [vmem((4 * block, hidden), BF16), blocks, blocks]
        + twice((8, block), (6, half), (half,), (4, half), (2, half // 2), (2, half))
        + [blocks, vmem((6, half, width), BF16), vmem((half, width), BF16)]
        + [vmem((2 * block, 128), F32), vmem((16, 1, 128), F32), vmem((8, 2 * block, 128), F32)]
        + [vmem((width, hidden), BF16)] * 2
        + [vmem((hidden, width), BF16), vmem((3, 8, hidden, cut), BF16)]
        + [vmem((block, width), BF16), vmem((block, 128), F32), flat, flat, turned, turned]
        + [ring, mine, ring, mine]
        + [vmem((k, hidden // h, cut), BF16) for k, h in ((4, 1), (2, 2), (2, 1))]
        + [vmem((8, width), F32), vmem((16, 1, width), F32), vmem((8, 1, width), F32)]
        + held
        + dma(6, 6, 25, 25, 25, 25, 25, 25, 14, 14, 10, 10, 15, 15, 7, 7, 15, 15),
        compiler_params=pltpu.CompilerParams(
            has_side_effects=True, vmem_limit_bytes=VMEM_LIMIT, collective_id=1
        ),
        name="step",
    )(
        tokens, targets, learner_gain.reshape(1, width), frozen_gain.reshape(1, width),
        learner_gate, learner_up, learner_down, frozen_gate, frozen_up, frozen_down,
    )
    scores, grad_tokens, grad_gain, grad_gate, grad_up, grad_down = pl.pallas_call(
        functools.partial(hand_over, len(shapes)),
        out_shape=shapes,
        in_specs=[away] * 6,
        out_specs=[away] * 6,
        scratch_shapes=held + [pltpu.SemaphoreType.DMA((2, 6))],
        name="hand_over",
    )(*results)
    return (
        scores.reshape(block),
        grad_tokens,
        grad_gain.reshape(width),
        grad_gate,
        grad_up,
        grad_down,
    )


def solution(mesh):
    placed = (
        P(("dp", "tensor"), None),
        P(("dp", "tensor"), None),
        P(),
        P(None, "tensor"),
        P(None, "tensor"),
        P("tensor", None),
        P(),
        P(None, "tensor"),
        P(None, "tensor"),
        P("tensor", None),
    )
    return jax.shard_map(
        local,
        mesh=mesh,
        in_specs=placed,
        out_specs=(
            P(("dp", "tensor")),
            P(("dp", "tensor"), None),
            P(),
            P("dp", "tensor"),
            P("dp", "tensor"),
            P("tensor", "dp"),
        ),
        check_vma=False,
    )
```

```python
import functools
import math

import jax
import jax.numpy as jnp
from jax import lax
from jax.experimental import pallas as pl
from jax.experimental.pallas import tpu as pltpu
from jax.sharding import PartitionSpec as P

F32 = jnp.float32
BF16 = jnp.bfloat16
MESH = pl.DeviceIdType.MESH
VMEM_LIMIT = 66_000_000
ROWS = 16


def digits(*order):
    return sum(p * 8**k for k, p in enumerate(order))


ARRIVAL = ((0,), (3, 1), (4,), (7, 2), (6, 5))
LATE = ((6, 2), (5, 3), (7, 4), (1, 0))
TERMS = digits(2, 6, 5, 3, 1, 7, 0, 4)
DOWN = digits(2, 1, 3, 0, 6, 5, 7, 4)
ALL, A, B, A0, A1, B0, B1 = (0, 4), (0, 2), (2, 4), (0, 1), (1, 2), (2, 3), (3, 4)


class Wires:
    def __init__(self, send_sem, recv_sems):
        self.send_sem, self.recv_sems = send_sem, recv_sems

    def copy(self, src, dst, into, device):
        return pltpu.make_async_remote_copy(
            src_ref=src,
            dst_ref=dst,
            send_sem=self.send_sem,
            recv_sem=self.recv_sems.at[into],
            device_id=device,
            device_id_type=MESH,
        )

    def send(self, src, dst, out, into, device):
        self.copy(src, dst, into, device).start()

    def got(self, ref, into, device):
        self.copy(ref, ref, into, device).wait_recv()

    def drain(self, ref, device):
        self.copy(ref, ref, 0, device).wait_send()


class Seat:
    def __init__(self):
        t = lax.axis_index("tensor")
        self.t = t
        self.z, self.y, self.c = t // 4, (t // 2) % 2, t % 2
        self.zp, self.zm, self.zf = (self.z + 1) % 4, (self.z + 3) % 4, (self.z + 2) % 4
        self.o, self.s = 1 - self.y, 1 - self.c

    def dev(self, z, y, c):
        return {"tensor": z * 4 + y * 2 + c}

    def pairs(self, i, chunks):
        return tuple(((self.z + p % 4) % 4) * 2 + (self.y + p // 4) % 2 for p in chunks[i])


def meet(devices):
    barrier = pltpu.get_barrier_semaphore()
    for device in devices:
        pl.semaphore_signal(barrier, inc=1, device_id=device, device_id_type=MESH)
    pl.semaphore_wait(barrier, len(devices))


class Gather:
    def __init__(self, seat, own, full, send_sems, recv_sems):
        self.s, self.own, self.full = seat, own, full
        self.w = Wires(send_sems, recv_sems)
        self.quarter = own.shape[0] // 4

    def rows(self, part):
        return pl.ds(part[0] * self.quarter, (part[1] - part[0]) * self.quarter)

    def blk(self, z, y, c, part):
        return self.full.at[z * 2 + y, c, self.rows(part)]

    def own_to(self, part, out, into, device):
        s = self.s
        self.w.send(self.own.at[self.rows(part)], self.blk(s.z, s.y, s.c, part), out, into, device)

    def pass_on(self, z, y, part, out, into, device):
        b = self.blk(z, y, self.s.c, part)
        self.w.send(b, b, out, into, device)

    def got(self, z, y, part, into):
        s = self.s
        self.w.got(self.blk(z, y, s.c, part), into, s.dev(s.z, s.y, s.s))

    def start(self):
        s = self.s
        up, down, across = s.dev(s.zp, s.y, s.c), s.dev(s.zm, s.y, s.c), s.dev(s.z, s.o, s.c)
        self.own_to(B, 0, 0, up)
        self.own_to(B, 1, 2, down)
        self.own_to(A, 2, 8, across)
        self.own_to(A, 3, 1, up)
        self.own_to(A, 4, 3, down)
        self.own_to(B, 5, 9, across)
        self.own_to(ALL, 6, 17, s.dev(s.z, s.y, s.s))
        self.full[s.z * 2 + s.y, s.c] = self.own[...]

    def arrive(self, *events):
        s = self.s
        z, zp, zm, zf, y, o = s.z, s.zp, s.zm, s.zf, s.y, s.o
        up, down, across = s.dev(zp, y, s.c), s.dev(zm, y, s.c), s.dev(z, o, s.c)
        sib = s.dev(z, y, s.s)
        for e in events:
            if e == 0:
                self.got(zm, y, B, 0)
                self.pass_on(zm, y, B0, 7, 4, up)
                self.pass_on(zm, y, B, 9, 11, across)
                self.got(zp, y, B, 2)
                self.pass_on(zp, y, B1, 8, 5, down)
                self.pass_on(zp, y, B, 10, 13, across)
            if e == 1:
                self.got(z, o, A, 8)
                self.pass_on(z, o, A, 12, 10, up)
                self.pass_on(z, o, A, 13, 12, down)
            if e == 2:
                self.got(zm, y, A, 1)
                self.pass_on(zm, y, A0, 14, 6, up)
                self.pass_on(zm, y, ALL, 18, 18, sib)
                self.got(zp, y, A, 3)
                self.pass_on(zp, y, A1, 15, 7, down)
                self.pass_on(zp, y, ALL, 19, 19, sib)
            if e == 3:
                self.got(z, o, B, 9)
                self.pass_on(z, o, ALL, 21, 21, sib)
            if e == 4:
                self.got(zf, y, B0, 4)
                self.got(zf, y, B1, 5)
                self.pass_on(zf, y, B, 11, 16, across)
            if e == 5:
                self.got(zm, o, A, 10)
                self.pass_on(zm, o, A0, 16, 14, up)
                self.got(zp, o, A, 12)
                self.pass_on(zp, o, A1, 17, 15, down)
            if e == 6:
                self.got(zf, y, A0, 6)
                self.got(zf, y, A1, 7)
                self.pass_on(zf, y, ALL, 20, 20, sib)
            if e == 7:
                self.got(zm, o, B, 11)
                self.pass_on(zm, o, ALL, 22, 22, sib)
            if e == 9:
                self.got(zp, o, B, 13)
                self.pass_on(zp, o, ALL, 23, 23, sib)
            if e == 8:
                self.got(zf, o, A0, 14)
                self.got(zf, o, A1, 15)
                self.got(zf, o, B, 16)
                self.pass_on(zf, o, ALL, 24, 24, sib)

    def have(self, i):
        s = self.s
        sib = s.dev(s.z, s.y, s.s)
        for place, p in zip(ARRIVAL[i], s.pairs(i, ARRIVAL)):
            self.w.got(self.full.at[p, s.s], (17, 19, 20, 18, 21, 23, 24, 22)[place], sib)


def fold(dst, refs):
    def rows(k, carry):
        at = pl.ds(pl.multiple_of(k * ROWS, ROWS), ROWS)
        dst[at] = total_of(refs, at).astype(dst.dtype)
        return carry

    lax.fori_loop(0, dst.shape[0] // ROWS, rows, 0)


class RingFirst:
    def __init__(self, block, dev, ring, row, slots, last, send_sems, recv_sems, base):
        self.block, self.dev, self.slots, self.last, self.base = block, dev, slots, last, base
        self.r, self.y, self.o = ring, row, 1 - row
        self.rp, self.rm, self.rf = (ring + 1) % 4, (ring + 3) % 4, (ring + 2) % 4
        self.w = Wires(send_sems, recv_sems)

    def out(self, r, y, slot, to, more=()):
        refs = self.block(r, y)
        if len(refs) + len(more) > 1:
            fold(refs[0], refs + [self.slots.at[k] for k in more])
        self.w.send(refs[0], self.slots.at[slot], self.base + slot, self.base + slot, to)

    def got(self, slot):
        self.w.got(self.slots.at[slot], self.base + slot, self.dev(self.rp, self.y))

    def ready(self, off, rel):
        up, down = self.dev(self.rp, self.y), self.dev(self.rm, self.y)
        if (off, rel) == (2, 1):
            self.out(self.rf, self.o, 0, up)
        if (off, rel) == (2, 0):
            self.out(self.rf, self.y, 1, down)
        if (off, rel) == (1, 0):
            self.out(self.rp, self.y, 3, up)
        if (off, rel) == (3, 1):
            self.out(self.rm, self.o, 4, down)

    def stage2(self):
        self.got(0)
        self.out(self.rp, self.o, 2, self.dev(self.rp, self.y), (0,))
        self.got(1)
        self.out(self.rm, self.y, 5, self.dev(self.rm, self.y), (1,))

    def stage3(self):
        self.got(4)
        self.got(2)
        refs = self.block(self.r, self.o)
        fold(refs[0], refs + [self.slots.at[2], self.slots.at[4]])
        self.w.send(refs[0], self.last, self.base + 6, self.base + 6, self.dev(self.r, self.o))

    def stage4(self):
        self.got(3)
        self.got(5)
        self.w.got(self.last, self.base + 6, self.dev(self.r, self.o))
        return self.block(self.r, self.y) + [self.slots.at[3], self.slots.at[5], self.last]


class RowFirst:
    def __init__(self, block, dev, ring, row, across, far, near, send_sems, recv_sems, base):
        self.block, self.dev, self.base = block, dev, base
        self.across, self.far, self.near = across, far, near
        self.r, self.y, self.o = ring, row, 1 - row
        self.rp, self.rm, self.rf = (ring + 1) % 4, (ring + 3) % 4, (ring + 2) % 4
        self.up, self.down, self.over = dev(self.rp, row), dev(self.rm, row), dev(ring, self.o)
        self.half = near.shape[1] // 2
        self.w = Wires(send_sems, recv_sems)

    def piece(self, ref, h):
        return ref.at[pl.ds(h * self.half, self.half)]

    def send(self, src, dst, k, to):
        self.w.send(src, dst, self.base + k, self.base + k, to)

    def got(self, ref, k):
        self.w.got(ref, self.base + k, self.over)

    def ready(self, off, rel):
        if rel == 1:
            r = (self.r + off) % 4
            refs = self.block(r, self.o)
            if len(refs) > 1:
                fold(refs[0], refs)
            self.send(refs[0], self.across.at[r], off, self.over)

    def joined(self, r, k):
        self.got(self.across.at[r], k)
        refs = self.block(r, self.y)
        fold(refs[0], refs + [self.across.at[r]])
        return refs[0]

    def far_out(self):
        ref = self.joined(self.rf, 2)
        self.send(self.piece(ref, 0), self.far.at[0], 4, self.up)
        self.send(self.piece(ref, 1), self.far.at[1], 5, self.down)

    def near_out(self):
        ref = self.joined(self.rp, 1)
        self.send(self.piece(ref, 1), self.piece(self.near.at[0], 1), 6, self.up)
        ref = self.joined(self.rm, 3)
        self.send(self.piece(ref, 0), self.piece(self.near.at[1], 0), 7, self.down)

    def stage3(self):
        self.got(self.far.at[0], 4)
        ref = self.piece(self.block(self.rp, self.y)[0], 0)
        fold(ref, [ref, self.far.at[0]])
        self.send(ref, self.piece(self.near.at[0], 0), 8, self.up)
        self.got(self.far.at[1], 5)
        ref = self.piece(self.block(self.rm, self.y)[0], 1)
        fold(ref, [ref, self.far.at[1]])
        self.send(ref, self.piece(self.near.at[1], 1), 9, self.down)

    def stage4(self):
        self.got(self.across.at[self.r], 0)
        for k, h, at in ((0, 1, 6), (1, 0, 7), (0, 0, 8), (1, 1, 9)):
            self.got(self.piece(self.near.at[k], h), at)
        return self.block(self.r, self.y) + [self.across.at[self.r], self.near.at[0], self.near.at[1]]


class GroupSum:
    def __init__(self, seat, chunks, partial, paired, ring_a, row_a, ring_b, send_sems, recv_sems):
        self.s, self.chunks, self.partial, self.paired = seat, chunks, partial, paired
        self.w = Wires(send_sems, recv_sems)
        half = paired.shape[1] // 2

        def block(h):
            at = pl.ds(h * half, half)
            return lambda z, y: [partial.at[z * 2 + y, seat.c, at], paired.at[z * 2 + y, at]]

        def dev(z, y):
            return seat.dev(z, y, seat.c)

        form, buffers = (RowFirst, row_a) if ring_a is None else (RingFirst, ring_a)
        self.a = form(block(0), dev, seat.z, seat.y, *buffers, send_sems, recv_sems, 15)
        self.b = RingFirst(block(1), dev, seat.z, seat.y, *ring_b, send_sems, recv_sems, 8)

    def places(self, i):
        first = sum(len(c) for c in self.chunks[:i])
        return [(first + j, p) for j, p in enumerate(self.s.pairs(i, self.chunks))]

    def pair_send(self, i):
        s = self.s
        for k, p in self.places(i):
            self.w.send(self.partial.at[p, s.s], self.paired.at[p], k, k, s.dev(s.z, s.y, s.s))

    def ready(self, i):
        s = self.s
        for k, p in self.places(i):
            self.w.got(self.paired.at[p], k, s.dev(s.z, s.y, s.s))
        for place in self.chunks[i]:
            self.b.ready(place % 4, place // 4)
            self.a.ready(place % 4, place // 4)


def total_of(refs, at):
    total = refs[0][at].astype(F32)
    for ref in refs[1:]:
        total = total + ref[at].astype(F32)
    return total


def sigmoid(v):
    return 1.0 / (1.0 + jnp.exp(-v))


def dot(a, b):
    return jnp.dot(a, b, preferred_element_type=F32)


def dot_t(a, b):
    return lax.dot_general(a, b, (((1,), (1,)), ((), ())), preferred_element_type=F32)


def tile(j, size):
    return pl.ds(pl.multiple_of(j * size, size), size)


def rows_of(ref, ps, at=slice(None)):
    parts = [ref[p, ..., at] for p in ps]
    return jnp.concatenate([v.reshape(-1, v.shape[-1]) for v in parts], axis=0)


def kernel(
    tokens, targets, lgain, fgain, wg, wu, wd, fg, fu, fd,
    scores, grad_tokens, grad_gain, out_gate, out_up, out_down,
    full, normed, fnormed, gate, up, hid_t, hid, lpart, fpart,
    lpaired, fpaired, lslots, fslots, llast, flast, lacross, facross, lfar, ffar, lnear, fnear,
    again, nslots, nlast, turn_w, row_w, col_w,
    vwg, vwu, vwd, terms, ograd, flat_scores,
    gg, ug, ggt, ugt, gslots, glast, uslots, ulast, dslots, dfar, dlast, gain_acc, gain_t, gain_d,
    o_scores, o_tokens, o_gain, o_gate, o_up, o_down,
    load_sems, out_sems, gsend, grecv, lsend, lrecv, fsend, frecv,
    qsend, qrecv, dsend, drecv, tsend, trecv, psend, precv, wsend, wrecv,
):
    seat = Seat()
    s = seat
    d = lax.axis_index("dp")
    x, yl = d % 4, d // 4
    block, width = tokens.shape
    hidden, cut = vwg.shape[1], terms.shape[3]
    deep, wide = width // hidden, hidden // cut
    n = 2 * block
    wt = 2 * cut
    moves = [(wg, vwg, 3), (wu, vwu, 4), (wd, vwd, 5)]
    for q, src in ((0, fg), (1, fu)):
        for j in range(wide):
            for k in range(deep):
                part = src.at[pl.ds(k * hidden, hidden), pl.ds(j * cut, cut)]
                moves.append((part, terms.at[q, j * deep + k], q))
    moves += [(fd.at[:, pl.ds(k * cut, cut)], terms.at[2, k], 2) for k in range(8)]

    def load(moves):
        for src, dst, k in moves:
            pltpu.make_async_copy(src, dst, load_sems.at[k]).start()

    def loaded(ref, k):
        pltpu.make_async_copy(ref, ref, load_sems.at[k]).wait()

    peers = [{"tensor": (s.t + r) % 16} for r in range(1, 16)]
    peers += [{"dp": (d + r) % 8} for r in range(1, 8)]
    load(moves[:3])
    meet(peers)
    gather = Gather(s, tokens, full, gsend.at[0], grecv)
    gather.start()
    load(moves[3:])
    ring_l, ring_f = (lslots, llast), (fslots, flast)
    row_l, row_f = (lacross, lfar, lnear), (facross, ffar, fnear)
    learner = GroupSum(s, ARRIVAL, lpart, lpaired, None, row_l, ring_l, lsend.at[0], lrecv)
    frozen = GroupSum(s, LATE, fpart, fpaired, None, row_f, ring_f, fsend.at[0], frecv)

    def unit(ref, at):
        v = ref[at].astype(F32)
        return v * lax.rsqrt(jnp.mean(v * v, axis=-1, keepdims=True) + 1e-05)

    def normalize(src, dst, gain):
        for k in range(block // ROWS):
            at = pl.ds(k * ROWS, ROWS)
            dst[at] = (unit(src, at) * gain[...]).astype(BF16)

    def frozen_units(i):
        for j, p in enumerate(s.pairs(i, LATE)):

            def one(core, carry, j=j, p=p):
                normalize(full.at[p, core], fnormed.at[j, core], fgain)
                return carry

            lax.fori_loop(0, 2, one, 0)

    def put(part, ps, cols, value):
        value = value.astype(BF16).reshape(len(ps), 2, block, value.shape[-1])
        for k, p in enumerate(ps):
            part[p, :, :, cols] = value[k]

    def frozen_hidden():
        def cols(j, carry):
            lhs = rows_of(fnormed, (0, 1))
            at = pl.ds(j * deep, deep)
            g = dot(lhs, terms[0, at].reshape(width, cut))
            u = dot(lhs, terms[1, at].reshape(width, cut))
            hid[:, tile(j, cut)] = (g * sigmoid(g) * u).astype(BF16)
            return carry

        lax.fori_loop(0, wide, cols, 0, unroll=True)

    def frozen_out(i):
        ps = s.pairs(i, LATE)

        def outs(j, carry):
            lhs = hid[...]
            value = jnp.concatenate([dot(lhs, terms[2, 2 * j + k]) for k in range(2)], axis=1)
            put(fpart, ps, tile(j, wt), value)
            return carry

        lax.fori_loop(0, 4, outs, 0, unroll=True)
        frozen.pair_send(i)

    def learner_units(i):
        for p in s.pairs(i, ARRIVAL):

            def one(core, carry, p=p):
                normalize(full.at[p, core], normed.at[p, core], lgain)
                return carry

            lax.fori_loop(0, 2, one, 0)

    def learner_hidden(i):
        ps = s.pairs(i, ARRIVAL)

        def cols(j, carry):
            at = tile(j, cut)
            lhs = rows_of(normed, ps)
            g, u = dot(lhs, vwg[:, at]), dot(lhs, vwu[:, at])
            h = g * sigmoid(g) * u
            hid[: n * len(ps), at] = h.astype(BF16)
            ht = h.T.astype(BF16)
            for k, p in enumerate(ps):
                mine = slice(k * n, k * n + n)
                gate[p, :, at], up[p, :, at] = g[mine], u[mine]
                hid_t[at, tile(p, n)] = ht[:, mine]
            return carry

        lax.fori_loop(0, wide, cols, 0, unroll=True)

    def learner_out(i):
        ps = s.pairs(i, ARRIVAL)

        def outs(j, carry):
            at = tile(j, wt)
            put(lpart, ps, at, dot(hid[: n * len(ps)], vwd[:, at]))
            return carry

        lax.fori_loop(0, width // wt, outs, 0, unroll=True)
        learner.pair_send(i)

    arrivals = (
        ((), (), (), ()),
        ((0, 1, 2), (3, 4), (), (5,)),
        ((), (7,), (), (6,)),
        ((), (9,), (8,), ()),
        ((), (), (), ()),
    )
    for i, events in enumerate(arrivals):
        gather.arrive(*events[0])
        gather.have(i)
        learner_units(i)
        gather.arrive(*events[1])
        if i == 0:
            for k, ref in ((3, vwg), (4, vwu), (5, vwd)):
                loaded(ref, k)
        if i > 0:
            learner.ready(i - 1)
        gather.arrive(*events[2])
        learner_hidden(i)
        gather.arrive(*events[3])
        learner_out(i)
    frozen_units(0)
    learner.ready(4)
    most = normed.at[:, :, :, pl.ds(0, width * 15 // 16)]
    sib = s.dev(s.z, s.y, s.s)
    gather.w.drain(most, sib)
    for q in range(3):
        loaded(terms.at[q], q)
    frozen_hidden()
    frozen_out(0)
    frozen_units(1)
    frozen_hidden()
    learner.b.stage2()
    learner.a.far_out()
    frozen.ready(0)
    frozen_out(1)
    frozen_units(2)
    learner.a.near_out()
    frozen.ready(1)
    frozen_hidden()
    learner.b.stage3()
    frozen_out(2)
    learner.a.stage3()
    frozen_units(3)
    frozen.ready(2)
    frozen.b.stage2()
    frozen_hidden()
    frozen.a.far_out()
    frozen_out(3)
    root = math.sqrt(width)

    def misses(refs, base):
        def rows(k, carry):
            at = pl.ds(pl.multiple_of(k * ROWS, ROWS), ROWS)
            here = pl.ds(pl.multiple_of(base + k * ROWS, ROWS), ROWS)
            miss = total_of(refs, at) - targets[here].astype(F32)
            loss = 0.5 * jnp.sum(miss * miss, axis=-1, keepdims=True) / root
            flat_scores[here] = jnp.broadcast_to(loss, (ROWS, flat_scores.shape[1]))
            ograd[here] = (miss / root).astype(BF16)
            return carry

        lax.fori_loop(0, block // 2 // ROWS, rows, 0)

    def weights(refs, base):
        def rows(k, carry):
            at = pl.ds(pl.multiple_of(k * ROWS, ROWS), ROWS)
            here = pl.ds(pl.multiple_of(base + k * ROWS, ROWS), ROWS)
            there = pl.ds(pl.multiple_of(s.c * block + base + k * ROWS, ROWS), ROWS)
            miss = total_of(refs, at) - targets[here].astype(F32)
            loss = 0.5 * jnp.sum(miss * miss, axis=-1, keepdims=True) / root
            score = flat_scores[here] - jnp.broadcast_to(loss, (ROWS, flat_scores.shape[1]))
            flat_scores[here] = score
            turn_w[there] = sigmoid(score)
            return carry

        lax.fori_loop(0, block // 2 // ROWS, rows, 0)

    misses(learner.a.stage4(), 0)
    misses(learner.b.stage4(), block // 2)
    regather = Gather(s, ograd, again, gsend.at[0], grecv)
    regather.start()
    frozen.ready(3)
    frozen.a.near_out()
    frozen.b.stage3()
    frozen.a.stage3()
    turn_w[...] = jnp.zeros_like(turn_w)
    outs = []

    def emit(src, dst):
        outs.append(pltpu.make_async_copy(src, dst, out_sems.at[len(outs)]))
        outs[-1].start()

    gain_acc[...] = jnp.zeros_like(gain_acc)

    learner.w.drain(most, sib)
    summed = GroupSum(s, LATE, lpart, lpaired, (nslots, nlast), None, ring_l, lsend.at[0], lrecv)

    def dp_dev(xx, yy):
        return {"dp": yy * 4 + xx}

    def dp_block(q):
        return lambda xx, yy: [terms.at[q, yy * 4 + xx]]

    gate_sum = RingFirst(dp_block(0), dp_dev, x, yl, gslots, glast, qsend.at[0], qrecv, 0)
    up_sum = RingFirst(dp_block(1), dp_dev, x, yl, uslots, ulast, qsend.at[1], qrecv, 7)
    down_sum = RowFirst(dp_block(2), dp_dev, x, yl, dslots, dfar, dlast, dsend.at[0], drecv, 0)

    def back(i):
        ps = s.pairs(i, ARRIVAL)

        def cols(j, carry):
            at = tile(j, cut)
            hg = dot_t(rows_of(again, ps), vwd[at, :])
            g, u = rows_of(gate, ps, at), rows_of(up, ps, at)
            sigma = sigmoid(g)
            side = hg * sigma
            ggrad = side * u * (1.0 + g * (1.0 - sigma))
            ugrad = side * g
            for value, plain, flipped in ((ggrad, gg, ggt), (ugrad, ug, ugt)):
                low, turned = value.astype(BF16), value.T.astype(BF16)
                for k, p in enumerate(ps):
                    mine = slice(k * n, k * n + n)
                    plain[p, :, at] = low[mine]
                    flipped[at, tile(p, n)] = turned[:, mine]
            return carry

        lax.fori_loop(0, wide, cols, 0, unroll=True)

    ww = Wires(wsend.at[0], wrecv)
    regather.arrive(0, 1)
    regather.have(0)
    back(0)
    regather.arrive(2)
    regather.have(1)
    back(1)
    regather.arrive(3, 4)
    weights(frozen.a.stage4(), 0)
    weights(frozen.b.stage4(), block // 2)
    row_w[s.t] = turn_w[...].T[:1]
    for r in range(1, 16):
        ww.send(row_w.at[s.t], row_w.at[s.t], r - 1, r - 1, {"tensor": (s.t + r) % 16})
    regather.arrive(5)
    regather.have(2)
    back(2)
    regather.arrive(7, 6, 9)
    regather.have(3)
    back(3)
    regather.arrive(8)
    regather.have(4)
    back(4)
    o_scores[...] = flat_scores[...].T[:1]
    for r in range(1, 16):
        ww.got(row_w.at[(s.t + 16 - r) % 16], r - 1, {"tensor": (s.t + 1) % 16})
    frozen.w.drain(most, sib)
    columns = jnp.concatenate([row_w[k] for k in range(16)], axis=0).T
    for p in range(8):
        both = columns[:, 2 * p : 2 * p + 1] + columns[:, 2 * p + 1 : 2 * p + 2]
        col_w[p] = jnp.broadcast_to(both, col_w.shape[1:])

    def weigh(ref):
        for p in range(8):
            at = pl.ds(p * n, n)
            ref[:, at] = (ref[:, at].astype(F32) * (row_w[2 * p] + row_w[2 * p + 1])).astype(BF16)

    def term(q, lhs, rhs, dd):
        at = tile(dd, cut)
        terms[q, dd] = dot(lhs[...], rhs[:, :, :, at].reshape(16 * block, cut)).astype(BF16)

    def some_terms(q, lhs, rhs, order, lo, hi):
        def one(k, code):
            row, ring = (yl + 1 + code % 8 // 4) % 2, (x + code % 4) % 4
            term(q, lhs, rhs, row * 4 + ring)
            return code // 8

        lax.fori_loop(lo, hi, one, jnp.int32(order // 8**lo), unroll=True)

    def normed_part(i):
        ps = s.pairs(i, LATE)

        def outs(j, carry):
            at = tile(j, wt)
            value = dot_t(rows_of(gg, ps), vwg[at, :]) + dot_t(rows_of(ug, ps), vwu[at, :])
            value = value * jnp.concatenate([col_w[p, :, :1] for p in ps], axis=0)
            put(lpart, ps, at, value)
            gains = value * rows_of(normed, ps, at).astype(F32)
            gain_acc[:, at] += gains.reshape(-1, 8, wt).sum(axis=0)
            return carry

        lax.fori_loop(0, width // wt, outs, 0, unroll=True)
        summed.pair_send(i)

    def ring_start(q, lhs, ring):
        some_terms(q, lhs, normed, TERMS, 0, 2)
        ring.ready(2, 1)
        ring.ready(2, 0)
        some_terms(q, lhs, normed, TERMS, 2, 4)
        ring.ready(1, 0)
        ring.ready(3, 1)

    weigh(ggt)
    ring_start(0, ggt, gate_sum)
    weigh(hid_t)
    some_terms(2, hid_t, again, DOWN, 0, 4)
    for off in (2, 1, 3, 0):
        down_sum.ready(off, 1)
    weigh(ugt)
    ring_start(1, ugt, up_sum)
    normed_part(0)
    normed_part(1)
    summed.ready(0)
    normed_part(2)
    summed.ready(1)
    normed_part(3)
    summed.ready(2)
    gain_t[s.t] = jnp.sum(gain_acc[...], axis=0, keepdims=True) / lgain[...]
    tw, pw = Wires(tsend.at[0], trecv), Wires(psend.at[0], precv)
    for r in range(1, 16):
        tw.send(gain_t.at[s.t], gain_t.at[s.t], r - 1, r - 1, {"tensor": (s.t + r) % 16})
    some_terms(0, ggt, normed, TERMS, 4, 8)
    gate_sum.stage2()
    summed.ready(3)
    summed.a.stage2()
    summed.b.stage2()
    some_terms(1, ugt, normed, TERMS, 4, 8)
    some_terms(2, hid_t, again, DOWN, 4, 8)
    up_sum.stage2()
    down_sum.far_out()
    down_sum.near_out()
    summed.a.stage3()
    summed.b.stage3()
    for r in range(1, 16):
        tw.got(gain_t.at[(s.t + 16 - r) % 16], r - 1, {"tensor": (s.t + 1) % 16})
    gain_d[d] = jnp.sum(gain_t[...], axis=0)
    for r in range(1, 8):
        pw.send(gain_d.at[d], gain_d.at[d], r - 1, r - 1, {"dp": (d + r) % 8})
    gate_sum.stage3()
    up_sum.stage3()
    down_sum.stage3()

    def token_grads(nrefs, base):
        def rows(k, carry):
            at = pl.ds(pl.multiple_of(k * ROWS, ROWS), ROWS)
            here = pl.ds(pl.multiple_of(base + k * ROWS, ROWS), ROWS)
            v = tokens[here].astype(F32)
            inv = lax.rsqrt(jnp.mean(v * v, axis=-1, keepdims=True) + 1e-05)
            scaled = total_of(nrefs, at) * lgain[...]
            mid = jnp.mean(scaled * v, axis=-1, keepdims=True)
            o_tokens[here] = (inv * scaled - v * (inv * inv * inv * mid)).astype(BF16)
            return carry

        lax.fori_loop(0, block // 2 // ROWS, rows, 0)

    token_grads(summed.a.stage4(), 0)
    token_grads(summed.b.stage4(), block // 2)
    emit(o_tokens, grad_tokens)
    for r in range(1, 8):
        pw.got(gain_d.at[(d + 8 - r) % 8], r - 1, {"dp": (d + 1) % 8})
    o_gain[...] = jnp.sum(gain_d[...], axis=0)
    emit(o_gain, grad_gain)
    emit(o_scores, scores)

    def finish_plain(out, refs):
        def rows(k, carry):
            at = pl.ds(pl.multiple_of(k * ROWS, ROWS), ROWS)
            out[at] = total_of(refs, at)
            return carry

        lax.fori_loop(0, hidden // ROWS, rows, 0)

    def finish_turned(out, refs):
        def rows(k, carry):
            at = tile(k, 128)
            out[:, at] = total_of(refs, at).T
            return carry

        lax.fori_loop(0, hidden // 128, rows, 0)

    finish_turned(o_gate, gate_sum.stage4())
    emit(o_gate, out_gate)
    finish_turned(o_up, up_sum.stage4())
    emit(o_up, out_up)
    finish_plain(o_down, down_sum.stage4())
    emit(o_down, out_down)
    for wires, ref in (
        (summed.w, most),
        (regather.w, most),
        (gate_sum.w, terms.at[0, pl.ds(0, 7)]),
        (up_sum.w, terms.at[1, pl.ds(0, 7)]),
        (down_sum.w, terms.at[2, pl.ds(0, 7)]),
        (tw, gain_t.at[pl.ds(0, 15)]),
        (pw, gain_d.at[pl.ds(0, 7)]),
        (ww, row_w.at[pl.ds(0, 15)]),
    ):
        wires.drain(ref, sib)
    for copy in outs:
        copy.wait()


def hand_over(count, *refs):
    srcs, dsts, held, sems = refs[:count], refs[count : 2 * count], refs[2 * count : -1], refs[-1]
    ins = [pltpu.make_async_copy(a, b, sems.at[0, k]) for k, (a, b) in enumerate(zip(srcs, held))]
    outs = [pltpu.make_async_copy(a, b, sems.at[1, k]) for k, (a, b) in enumerate(zip(held, dsts))]
    for copy in ins:
        copy.start()
    for copy, then in zip(ins, outs):
        copy.wait()
        then.start()
    for copy in outs:
        copy.wait()


def local(
    tokens, targets, learner_gain, learner_gate, learner_up, learner_down,
    frozen_gain, frozen_gate, frozen_up, frozen_down,
):
    block, width = tokens.shape
    hidden = learner_gate.shape[1]
    cut, group, half = width // 8, 16 * block, block // 2
    here = pl.BlockSpec(memory_space=pltpu.VMEM)
    away = pl.BlockSpec(memory_space=pl.ANY)
    shape, vmem = jax.ShapeDtypeStruct, pltpu.VMEM

    def dma(*counts):
        return [pltpu.SemaphoreType.DMA((k,)) for k in counts]

    def twice(*shapes):
        return [vmem((*lead, width), BF16) for lead in shapes for _ in range(2)]

    blocks = vmem((8, 2, block, width), BF16)
    pre = vmem((8, 2 * block, hidden), F32)
    flat = vmem((8, 2 * block, hidden), BF16)
    turned = vmem((hidden, group), BF16)
    ring, mine = vmem((6, hidden, cut), BF16), vmem((hidden, cut), BF16)
    shapes = (
        shape((1, block), F32),
        shape((block, width), BF16),
        shape((1, width), F32),
        shape((cut, hidden), F32),
        shape((cut, hidden), F32),
        shape((hidden, cut), F32),
    )
    held = [vmem(a.shape, a.dtype) for a in shapes]
    results = pl.pallas_call(
        kernel,
        out_shape=shapes,
        in_specs=[here] * 4 + [away] * 6,
        out_specs=[away] * 6,
        scratch_shapes=[blocks, blocks, vmem((2, 2, block, width), BF16), pre, pre, turned]
        + [vmem((4 * block, hidden), BF16), blocks, blocks]
        + twice((8, block), (6, half), (half,), (4, half), (2, half // 2), (2, half))
        + [blocks, vmem((6, half, width), BF16), vmem((half, width), BF16)]
        + [vmem((2 * block, 128), F32), vmem((16, 1, 128), F32), vmem((8, 2 * block, 128), F32)]
        + [vmem((width, hidden), BF16)] * 2
        + [vmem((hidden, width), BF16), vmem((3, 8, hidden, cut), BF16)]
        + [vmem((block, width), BF16), vmem((block, 128), F32), flat, flat, turned, turned]
        + [ring, mine, ring, mine]
        + [vmem((k, hidden // h, cut), BF16) for k, h in ((4, 1), (2, 2), (2, 1))]
        + [vmem((8, width), F32), vmem((16, 1, width), F32), vmem((8, 1, width), F32)]
        + held
        + dma(6, 6, 1, 25, 1, 25, 1, 25, 2, 14, 1, 10, 1, 15, 1, 7, 1, 15),
        compiler_params=pltpu.CompilerParams(
            has_side_effects=True, vmem_limit_bytes=VMEM_LIMIT, collective_id=1
        ),
        name="step",
    )(
        tokens, targets, learner_gain.reshape(1, width), frozen_gain.reshape(1, width),
        learner_gate, learner_up, learner_down, frozen_gate, frozen_up, frozen_down,
    )
    scores, grad_tokens, grad_gain, grad_gate, grad_up, grad_down = pl.pallas_call(
        functools.partial(hand_over, len(shapes)),
        out_shape=shapes,
        in_specs=[away] * 6,
        out_specs=[away] * 6,
        scratch_shapes=held + [pltpu.SemaphoreType.DMA((2, 6))],
        name="hand_over",
    )(*results)
    return (
        scores.reshape(block),
        grad_tokens,
        grad_gain.reshape(width),
        grad_gate,
        grad_up,
        grad_down,
    )


def solution(mesh):
    placed = (
        P(("dp", "tensor"), None),
        P(("dp", "tensor"), None),
        P(),
        P(None, "tensor"),
        P(None, "tensor"),
        P("tensor", None),
        P(),
        P(None, "tensor"),
        P(None, "tensor"),
        P("tensor", None),
    )
    return jax.shard_map(
        local,
        mesh=mesh,
        in_specs=placed,
        out_specs=(
            P(("dp", "tensor")),
            P(("dp", "tensor"), None),
            P(),
            P("dp", "tensor"),
            P("dp", "tensor"),
            P("tensor", "dp"),
        ),
        check_vma=False,
    )
```

```python
import functools
import math

import jax
import jax.numpy as jnp
from jax import lax
from jax.experimental import pallas as pl
from jax.experimental.pallas import tpu as pltpu
from jax.sharding import PartitionSpec as P

F32 = jnp.float32
BF16 = jnp.bfloat16
MESH = pl.DeviceIdType.MESH
VMEM_LIMIT = 66_000_000
ROWS = 16


def digits(*order):
    return sum(p * 8**k for k, p in enumerate(order))


ARRIVAL = ((0,), (3, 1), (4,), (7, 2), (6, 5))
LATE = ((6, 2), (5, 3), (7, 4), (1, 0))
TERMS = digits(2, 6, 5, 3, 1, 7, 0, 4)
DOWN = digits(2, 1, 3, 0, 6, 5, 7, 4)
ALL, A, B, A0, A1, B0, B1 = (0, 4), (0, 2), (2, 4), (0, 1), (1, 2), (2, 3), (3, 4)


class Wires:
    def __init__(self, send_sem, recv_sems):
        self.send_sem, self.recv_sems = send_sem, recv_sems

    def copy(self, src, dst, into, device):
        return pltpu.make_async_remote_copy(
            src_ref=src,
            dst_ref=dst,
            send_sem=self.send_sem,
            recv_sem=self.recv_sems.at[into],
            device_id=device,
            device_id_type=MESH,
        )

    def send(self, src, dst, out, into, device):
        self.copy(src, dst, into, device).start()

    def got(self, ref, into, device):
        self.copy(ref, ref, into, device).wait_recv()

    def drain(self, ref, device):
        self.copy(ref, ref, 0, device).wait_send()


class Seat:
    def __init__(self):
        t = lax.axis_index("tensor")
        self.t = t
        self.z, self.y, self.c = t // 4, (t // 2) % 2, t % 2
        self.zp, self.zm, self.zf = (self.z + 1) % 4, (self.z + 3) % 4, (self.z + 2) % 4
        self.o, self.s = 1 - self.y, 1 - self.c

    def dev(self, z, y, c):
        return {"tensor": z * 4 + y * 2 + c}

    def pairs(self, i, chunks):
        return tuple(((self.z + p % 4) % 4) * 2 + (self.y + p // 4) % 2 for p in chunks[i])


def meet(devices):
    barrier = pltpu.get_barrier_semaphore()
    for device in devices:
        pl.semaphore_signal(barrier, inc=1, device_id=device, device_id_type=MESH)
    pl.semaphore_wait(barrier, len(devices))


class Gather:
    def __init__(self, seat, own, full, send_sems, recv_sems):
        self.s, self.own, self.full = seat, own, full
        self.w = Wires(send_sems, recv_sems)
        self.quarter = own.shape[0] // 4

    def rows(self, part):
        return pl.ds(part[0] * self.quarter, (part[1] - part[0]) * self.quarter)

    def blk(self, z, y, c, part):
        return self.full.at[z * 2 + y, c, self.rows(part)]

    def own_to(self, part, out, into, device):
        s = self.s
        self.w.send(self.own.at[self.rows(part)], self.blk(s.z, s.y, s.c, part), out, into, device)

    def pass_on(self, z, y, part, out, into, device):
        b = self.blk(z, y, self.s.c, part)
        self.w.send(b, b, out, into, device)

    def got(self, z, y, part, into):
        s = self.s
        self.w.got(self.blk(z, y, s.c, part), into, s.dev(s.z, s.y, s.s))

    def start(self):
        s = self.s
        up, down, across = s.dev(s.zp, s.y, s.c), s.dev(s.zm, s.y, s.c), s.dev(s.z, s.o, s.c)
        self.own_to(B, 0, 0, up)
        self.own_to(B, 1, 2, down)
        self.own_to(A, 2, 8, across)
        self.own_to(A, 3, 1, up)
        self.own_to(A, 4, 3, down)
        self.own_to(B, 5, 9, across)
        self.own_to(ALL, 6, 17, s.dev(s.z, s.y, s.s))
        self.full[s.z * 2 + s.y, s.c] = self.own[...]

    def arrive(self, *events):
        s = self.s
        z, zp, zm, zf, y, o = s.z, s.zp, s.zm, s.zf, s.y, s.o
        up, down, across = s.dev(zp, y, s.c), s.dev(zm, y, s.c), s.dev(z, o, s.c)
        sib = s.dev(z, y, s.s)
        for e in events:
            if e == 0:
                self.got(zm, y, B, 0)
                self.pass_on(zm, y, B0, 7, 4, up)
                self.pass_on(zm, y, B, 9, 11, across)
                self.got(zp, y, B, 2)
                self.pass_on(zp, y, B1, 8, 5, down)
                self.pass_on(zp, y, B, 10, 13, across)
            if e == 1:
                self.got(z, o, A, 8)
                self.pass_on(z, o, A, 12, 10, up)
                self.pass_on(z, o, A, 13, 12, down)
            if e == 2:
                self.got(zm, y, A, 1)
                self.pass_on(zm, y, A0, 14, 6, up)
                self.pass_on(zm, y, ALL, 18, 18, sib)
                self.got(zp, y, A, 3)
                self.pass_on(zp, y, A1, 15, 7, down)
                self.pass_on(zp, y, ALL, 19, 19, sib)
            if e == 3:
                self.got(z, o, B, 9)
                self.pass_on(z, o, ALL, 21, 21, sib)
            if e == 4:
                self.got(zf, y, B0, 4)
                self.got(zf, y, B1, 5)
                self.pass_on(zf, y, B, 11, 16, across)
            if e == 5:
                self.got(zm, o, A, 10)
                self.pass_on(zm, o, A0, 16, 14, up)
                self.got(zp, o, A, 12)
                self.pass_on(zp, o, A1, 17, 15, down)
            if e == 6:
                self.got(zf, y, A0, 6)
                self.got(zf, y, A1, 7)
                self.pass_on(zf, y, ALL, 20, 20, sib)
            if e == 7:
                self.got(zm, o, B, 11)
                self.pass_on(zm, o, ALL, 22, 22, sib)
            if e == 9:
                self.got(zp, o, B, 13)
                self.pass_on(zp, o, ALL, 23, 23, sib)
            if e == 8:
                self.got(zf, o, A0, 14)
                self.got(zf, o, A1, 15)
                self.got(zf, o, B, 16)
                self.pass_on(zf, o, ALL, 24, 24, sib)

    def have(self, i):
        s = self.s
        sib = s.dev(s.z, s.y, s.s)
        for place, p in zip(ARRIVAL[i], s.pairs(i, ARRIVAL)):
            self.w.got(self.full.at[p, s.s], (17, 19, 20, 18, 21, 23, 24, 22)[place], sib)


def fold(dst, refs):
    def rows(k, carry):
        at = pl.ds(pl.multiple_of(k * ROWS, ROWS), ROWS)
        dst[at] = total_of(refs, at).astype(dst.dtype)
        return carry

    lax.fori_loop(0, dst.shape[0] // ROWS, rows, 0)


class RingFirst:
    def __init__(self, block, dev, ring, row, slots, last, send_sems, recv_sems, base):
        self.block, self.dev, self.slots, self.last, self.base = block, dev, slots, last, base
        self.r, self.y, self.o = ring, row, 1 - row
        self.rp, self.rm, self.rf = (ring + 1) % 4, (ring + 3) % 4, (ring + 2) % 4
        self.w = Wires(send_sems, recv_sems)

    def out(self, r, y, slot, to, more=()):
        refs = self.block(r, y)
        if len(refs) + len(more) > 1:
            fold(refs[0], refs + [self.slots.at[k] for k in more])
        self.w.send(refs[0], self.slots.at[slot], self.base + slot, self.base + slot, to)

    def got(self, slot):
        self.w.got(self.slots.at[slot], self.base + slot, self.dev(self.rp, self.y))

    def ready(self, off, rel):
        up, down = self.dev(self.rp, self.y), self.dev(self.rm, self.y)
        if (off, rel) == (2, 1):
            self.out(self.rf, self.o, 0, up)
        if (off, rel) == (2, 0):
            self.out(self.rf, self.y, 1, down)
        if (off, rel) == (1, 0):
            self.out(self.rp, self.y, 3, up)
        if (off, rel) == (3, 1):
            self.out(self.rm, self.o, 4, down)

    def stage2(self):
        self.got(0)
        self.out(self.rp, self.o, 2, self.dev(self.rp, self.y), (0,))
        self.got(1)
        self.out(self.rm, self.y, 5, self.dev(self.rm, self.y), (1,))

    def stage3(self):
        self.got(4)
        self.got(2)
        refs = self.block(self.r, self.o)
        fold(refs[0], refs + [self.slots.at[2], self.slots.at[4]])
        self.w.send(refs[0], self.last, self.base + 6, self.base + 6, self.dev(self.r, self.o))

    def stage4(self):
        self.got(3)
        self.got(5)
        self.w.got(self.last, self.base + 6, self.dev(self.r, self.o))
        return self.block(self.r, self.y) + [self.slots.at[3], self.slots.at[5], self.last]


class RowFirst:
    def __init__(self, block, dev, ring, row, across, far, near, send_sems, recv_sems, base):
        self.block, self.dev, self.base = block, dev, base
        self.across, self.far, self.near = across, far, near
        self.r, self.y, self.o = ring, row, 1 - row
        self.rp, self.rm, self.rf = (ring + 1) % 4, (ring + 3) % 4, (ring + 2) % 4
        self.up, self.down, self.over = dev(self.rp, row), dev(self.rm, row), dev(ring, self.o)
        self.half = near.shape[1] // 2
        self.w = Wires(send_sems, recv_sems)

    def piece(self, ref, h):
        return ref.at[pl.ds(h * self.half, self.half)]

    def send(self, src, dst, k, to):
        self.w.send(src, dst, self.base + k, self.base + k, to)

    def got(self, ref, k):
        self.w.got(ref, self.base + k, self.over)

    def ready(self, off, rel):
        if rel == 1:
            r = (self.r + off) % 4
            refs = self.block(r, self.o)
            if len(refs) > 1:
                fold(refs[0], refs)
            self.send(refs[0], self.across.at[r], off, self.over)

    def joined(self, r, k):
        self.got(self.across.at[r], k)
        refs = self.block(r, self.y)
        fold(refs[0], refs + [self.across.at[r]])
        return refs[0]

    def far_out(self):
        ref = self.joined(self.rf, 2)
        self.send(self.piece(ref, 0), self.far.at[0], 4, self.up)
        self.send(self.piece(ref, 1), self.far.at[1], 5, self.down)

    def near_out(self):
        ref = self.joined(self.rp, 1)
        self.send(self.piece(ref, 1), self.piece(self.near.at[0], 1), 6, self.up)
        ref = self.joined(self.rm, 3)
        self.send(self.piece(ref, 0), self.piece(self.near.at[1], 0), 7, self.down)

    def stage3(self):
        self.got(self.far.at[0], 4)
        ref = self.piece(self.block(self.rp, self.y)[0], 0)
        fold(ref, [ref, self.far.at[0]])
        self.send(ref, self.piece(self.near.at[0], 0), 8, self.up)
        self.got(self.far.at[1], 5)
        ref = self.piece(self.block(self.rm, self.y)[0], 1)
        fold(ref, [ref, self.far.at[1]])
        self.send(ref, self.piece(self.near.at[1], 1), 9, self.down)

    def stage4(self):
        self.got(self.across.at[self.r], 0)
        for k, h, at in ((0, 1, 6), (1, 0, 7), (0, 0, 8), (1, 1, 9)):
            self.got(self.piece(self.near.at[k], h), at)
        return self.block(self.r, self.y) + [self.across.at[self.r], self.near.at[0], self.near.at[1]]


class GroupSum:
    def __init__(self, seat, chunks, partial, paired, ring_a, row_a, ring_b, send_sems, recv_sems):
        self.s, self.chunks, self.partial, self.paired = seat, chunks, partial, paired
        self.w = Wires(send_sems, recv_sems)
        half = paired.shape[1] // 2

        def block(h):
            at = pl.ds(h * half, half)
            return lambda z, y: [partial.at[z * 2 + y, seat.c, at], paired.at[z * 2 + y, at]]

        def dev(z, y):
            return seat.dev(z, y, seat.c)

        form, buffers = (RowFirst, row_a) if ring_a is None else (RingFirst, ring_a)
        self.a = form(block(0), dev, seat.z, seat.y, *buffers, send_sems, recv_sems, 15)
        self.b = RingFirst(block(1), dev, seat.z, seat.y, *ring_b, send_sems, recv_sems, 8)

    def places(self, i):
        first = sum(len(c) for c in self.chunks[:i])
        return [(first + j, p) for j, p in enumerate(self.s.pairs(i, self.chunks))]

    def pair_send(self, i):
        s = self.s
        for k, p in self.places(i):
            self.w.send(self.partial.at[p, s.s], self.paired.at[p], k, k, s.dev(s.z, s.y, s.s))

    def ready(self, i):
        s = self.s
        for k, p in self.places(i):
            self.w.got(self.paired.at[p], k, s.dev(s.z, s.y, s.s))
        for place in self.chunks[i]:
            self.b.ready(place % 4, place // 4)
            self.a.ready(place % 4, place // 4)


def total_of(refs, at):
    total = refs[0][at].astype(F32)
    for ref in refs[1:]:
        total = total + ref[at].astype(F32)
    return total


def sigmoid(v):
    return 1.0 / (1.0 + jnp.exp(-v))


def dot(a, b):
    return jnp.dot(a, b, preferred_element_type=F32)


def dot_t(a, b):
    return lax.dot_general(a, b, (((1,), (1,)), ((), ())), preferred_element_type=F32)


def tile(j, size):
    return pl.ds(pl.multiple_of(j * size, size), size)


def rows_of(ref, ps, at=slice(None)):
    parts = [ref[p, ..., at] for p in ps]
    return jnp.concatenate([v.reshape(-1, v.shape[-1]) for v in parts], axis=0)


def kernel(
    tokens_in, targets_in, lgain_in, fgain_in, wg, wu, wd, fg, fu, fd,
    scores, grad_tokens, grad_gain, out_gate, out_up, out_down,
    full, normed, fnormed, gate, up, hid_t, hid, lpart, fpart,
    lpaired, fpaired, lslots, fslots, llast, flast, lacross, facross, lfar, ffar, lnear, fnear,
    again, nslots, nlast, turn_w, row_w, col_w, tokens, targets, lgain, fgain,
    vwg, vwu, vwd, terms, ograd, flat_scores,
    gg, ug, ggt, ugt, gslots, glast, uslots, ulast, dslots, dfar, dlast, gain_acc, gain_t, gain_d,
    o_scores, o_tokens, o_gain, o_gate, o_up, o_down,
    load_sems, out_sems, gsend, grecv, lsend, lrecv, fsend, frecv,
    qsend, qrecv, dsend, drecv, tsend, trecv, psend, precv, wsend, wrecv,
):
    seat = Seat()
    s = seat
    d = lax.axis_index("dp")
    x, yl = d % 4, d // 4
    block, width = tokens.shape
    hidden, cut = vwg.shape[1], terms.shape[3]
    deep, wide = width // hidden, hidden // cut
    n = 2 * block
    wt = 2 * cut
    small = [(tokens_in, tokens, 6), (lgain_in, lgain, 7), (fgain_in, fgain, 8)]
    small.append((targets_in, targets, 9))
    moves = [(wg, vwg, 3), (wu, vwu, 4), (wd, vwd, 5)]
    for q, src in ((0, fg), (1, fu)):
        for j in range(wide):
            for k in range(deep):
                part = src.at[pl.ds(k * hidden, hidden), pl.ds(j * cut, cut)]
                moves.append((part, terms.at[q, j * deep + k], q))
    moves += [(fd.at[:, pl.ds(k * cut, cut)], terms.at[2, k], 2) for k in range(8)]

    def load(moves):
        for src, dst, k in moves:
            pltpu.make_async_copy(src, dst, load_sems.at[k]).start()

    def loaded(ref, k):
        pltpu.make_async_copy(ref, ref, load_sems.at[k]).wait()

    peers = [{"tensor": (s.t + r) % 16} for r in range(1, 16)]
    peers += [{"dp": (d + r) % 8} for r in range(1, 8)]
    load(small)
    load(moves[:3])
    meet(peers)
    loaded(tokens, 6)
    gather = Gather(s, tokens, full, gsend.at[0], grecv)
    gather.start()
    load(moves[3:])
    loaded(lgain, 7)
    loaded(fgain, 8)
    loaded(targets, 9)
    ring_l, ring_f = (lslots, llast), (fslots, flast)
    row_l, row_f = (lacross, lfar, lnear), (facross, ffar, fnear)
    learner = GroupSum(s, ARRIVAL, lpart, lpaired, None, row_l, ring_l, lsend.at[0], lrecv)
    frozen = GroupSum(s, LATE, fpart, fpaired, None, row_f, ring_f, fsend.at[0], frecv)

    def unit(ref, at):
        v = ref[at].astype(F32)
        return v * lax.rsqrt(jnp.mean(v * v, axis=-1, keepdims=True) + 1e-05)

    def normalize(src, dst, gain):
        for k in range(block // ROWS):
            at = pl.ds(k * ROWS, ROWS)
            dst[at] = (unit(src, at) * gain[...]).astype(BF16)

    def frozen_units(i):
        for j, p in enumerate(s.pairs(i, LATE)):

            def one(core, carry, j=j, p=p):
                normalize(full.at[p, core], fnormed.at[j, core], fgain)
                return carry

            lax.fori_loop(0, 2, one, 0)

    def put(part, ps, cols, value):
        value = value.astype(BF16).reshape(len(ps), 2, block, value.shape[-1])
        for k, p in enumerate(ps):
            part[p, :, :, cols] = value[k]

    def frozen_hidden():
        def cols(j, carry):
            lhs = rows_of(fnormed, (0, 1))
            at = pl.ds(j * deep, deep)
            g = dot(lhs, terms[0, at].reshape(width, cut))
            u = dot(lhs, terms[1, at].reshape(width, cut))
            hid[:, tile(j, cut)] = (g * sigmoid(g) * u).astype(BF16)
            return carry

        lax.fori_loop(0, wide, cols, 0, unroll=True)

    def frozen_out(i):
        ps = s.pairs(i, LATE)

        def outs(j, carry):
            lhs = hid[...]
            value = jnp.concatenate([dot(lhs, terms[2, 2 * j + k]) for k in range(2)], axis=1)
            put(fpart, ps, tile(j, wt), value)
            return carry

        lax.fori_loop(0, 4, outs, 0, unroll=True)
        frozen.pair_send(i)

    def learner_units(i):
        for p in s.pairs(i, ARRIVAL):

            def one(core, carry, p=p):
                normalize(full.at[p, core], normed.at[p, core], lgain)
                return carry

            lax.fori_loop(0, 2, one, 0)

    def learner_hidden(i):
        ps = s.pairs(i, ARRIVAL)

        def cols(j, carry):
            at = tile(j, cut)
            lhs = rows_of(normed, ps)
            g, u = dot(lhs, vwg[:, at]), dot(lhs, vwu[:, at])
            h = g * sigmoid(g) * u
            hid[: n * len(ps), at] = h.astype(BF16)
            ht = h.T.astype(BF16)
            for k, p in enumerate(ps):
                mine = slice(k * n, k * n + n)
                gate[p, :, at], up[p, :, at] = g[mine], u[mine]
                hid_t[at, tile(p, n)] = ht[:, mine]
            return carry

        lax.fori_loop(0, wide, cols, 0, unroll=True)

    def learner_out(i):
        ps = s.pairs(i, ARRIVAL)

        def outs(j, carry):
            at = tile(j, wt)
            put(lpart, ps, at, dot(hid[: n * len(ps)], vwd[:, at]))
            return carry

        lax.fori_loop(0, width // wt, outs, 0, unroll=True)
        learner.pair_send(i)

    arrivals = (
        ((), (), (), ()),
        ((0, 1, 2), (3, 4), (), (5,)),
        ((), (7,), (), (6,)),
        ((), (9,), (8,), ()),
        ((), (), (), ()),
    )
    for i, events in enumerate(arrivals):
        gather.arrive(*events[0])
        gather.have(i)
        learner_units(i)
        gather.arrive(*events[1])
        if i == 0:
            for k, ref in ((3, vwg), (4, vwu), (5, vwd)):
                loaded(ref, k)
        if i > 0:
            learner.ready(i - 1)
        gather.arrive(*events[2])
        learner_hidden(i)
        gather.arrive(*events[3])
        learner_out(i)
    frozen_units(0)
    learner.ready(4)
    most = normed.at[:, :, :, pl.ds(0, width * 15 // 16)]
    sib = s.dev(s.z, s.y, s.s)
    gather.w.drain(most, sib)
    for q in range(3):
        loaded(terms.at[q], q)
    frozen_hidden()
    frozen_out(0)
    frozen_units(1)
    frozen_hidden()
    learner.b.stage2()
    learner.a.far_out()
    frozen.ready(0)
    frozen_out(1)
    frozen_units(2)
    learner.a.near_out()
    frozen.ready(1)
    frozen_hidden()
    learner.b.stage3()
    frozen_out(2)
    learner.a.stage3()
    frozen_units(3)
    frozen.ready(2)
    frozen.b.stage2()
    frozen_hidden()
    frozen.a.far_out()
    frozen_out(3)
    root = math.sqrt(width)

    def misses(refs, base):
        def rows(k, carry):
            at = pl.ds(pl.multiple_of(k * ROWS, ROWS), ROWS)
            here = pl.ds(pl.multiple_of(base + k * ROWS, ROWS), ROWS)
            miss = total_of(refs, at) - targets[here].astype(F32)
            loss = 0.5 * jnp.sum(miss * miss, axis=-1, keepdims=True) / root
            flat_scores[here] = jnp.broadcast_to(loss, (ROWS, flat_scores.shape[1]))
            ograd[here] = (miss / root).astype(BF16)
            return carry

        lax.fori_loop(0, block // 2 // ROWS, rows, 0)

    def weights(refs, base):
        def rows(k, carry):
            at = pl.ds(pl.multiple_of(k * ROWS, ROWS), ROWS)
            here = pl.ds(pl.multiple_of(base + k * ROWS, ROWS), ROWS)
            there = pl.ds(pl.multiple_of(s.c * block + base + k * ROWS, ROWS), ROWS)
            miss = total_of(refs, at) - targets[here].astype(F32)
            loss = 0.5 * jnp.sum(miss * miss, axis=-1, keepdims=True) / root
            score = flat_scores[here] - jnp.broadcast_to(loss, (ROWS, flat_scores.shape[1]))
            flat_scores[here] = score
            turn_w[there] = sigmoid(score)
            return carry

        lax.fori_loop(0, block // 2 // ROWS, rows, 0)

    misses(learner.a.stage4(), 0)
    misses(learner.b.stage4(), block // 2)
    regather = Gather(s, ograd, again, gsend.at[0], grecv)
    regather.start()
    frozen.ready(3)
    frozen.a.near_out()
    frozen.b.stage3()
    frozen.a.stage3()
    turn_w[...] = jnp.zeros_like(turn_w)
    outs = []

    def emit(src, dst):
        outs.append(pltpu.make_async_copy(src, dst, out_sems.at[len(outs)]))
        outs[-1].start()

    gain_acc[...] = jnp.zeros_like(gain_acc)

    learner.w.drain(most, sib)
    summed = GroupSum(s, LATE, lpart, lpaired, (nslots, nlast), None, ring_l, lsend.at[0], lrecv)

    def dp_dev(xx, yy):
        return {"dp": yy * 4 + xx}

    def dp_block(q):
        return lambda xx, yy: [terms.at[q, yy * 4 + xx]]

    gate_sum = RingFirst(dp_block(0), dp_dev, x, yl, gslots, glast, qsend.at[0], qrecv, 0)
    up_sum = RingFirst(dp_block(1), dp_dev, x, yl, uslots, ulast, qsend.at[1], qrecv, 7)
    down_sum = RowFirst(dp_block(2), dp_dev, x, yl, dslots, dfar, dlast, dsend.at[0], drecv, 0)

    def back(i):
        ps = s.pairs(i, ARRIVAL)

        def cols(j, carry):
            at = tile(j, cut)
            hg = dot_t(rows_of(again, ps), vwd[at, :])
            g, u = rows_of(gate, ps, at), rows_of(up, ps, at)
            sigma = sigmoid(g)
            side = hg * sigma
            ggrad = side * u * (1.0 + g * (1.0 - sigma))
            ugrad = side * g
            for value, plain, flipped in ((ggrad, gg, ggt), (ugrad, ug, ugt)):
                low, turned = value.astype(BF16), value.T.astype(BF16)
                for k, p in enumerate(ps):
                    mine = slice(k * n, k * n + n)
                    plain[p, :, at] = low[mine]
                    flipped[at, tile(p, n)] = turned[:, mine]
            return carry

        lax.fori_loop(0, wide, cols, 0, unroll=True)

    ww = Wires(wsend.at[0], wrecv)
    regather.arrive(0, 1)
    regather.have(0)
    back(0)
    regather.arrive(2)
    regather.have(1)
    back(1)
    regather.arrive(3, 4)
    weights(frozen.a.stage4(), 0)
    weights(frozen.b.stage4(), block // 2)
    row_w[s.t] = turn_w[...].T[:1]
    for r in range(1, 16):
        ww.send(row_w.at[s.t], row_w.at[s.t], 0, 0, {"tensor": (s.t + r) % 16})
    regather.arrive(5)
    regather.have(2)
    back(2)
    regather.arrive(7, 6, 9)
    regather.have(3)
    back(3)
    regather.arrive(8)
    regather.have(4)
    back(4)
    ww.got(row_w.at[pl.ds(0, 15)], 0, sib)
    def weigh(ref):
        for p in range(8):
            at = pl.ds(p * n, n)
            ref[:, at] = (ref[:, at].astype(F32) * (row_w[2 * p] + row_w[2 * p + 1])).astype(BF16)

    def term(q, lhs, rhs, dd):
        at = tile(dd, cut)
        terms[q, dd] = dot(lhs[...], rhs[:, :, :, at].reshape(16 * block, cut)).astype(BF16)

    def some_terms(q, lhs, rhs, order, lo, hi):
        def one(k, code):
            row, ring = (yl + 1 + code % 8 // 4) % 2, (x + code % 4) % 4
            term(q, lhs, rhs, row * 4 + ring)
            return code // 8

        lax.fori_loop(lo, hi, one, jnp.int32(order // 8**lo), unroll=True)

    def normed_part(i):
        ps = s.pairs(i, LATE)

        def outs(j, carry):
            at = tile(j, wt)
            value = dot_t(rows_of(gg, ps), vwg[at, :]) + dot_t(rows_of(ug, ps), vwu[at, :])
            value = value * jnp.concatenate([col_w[p, :, :1] for p in ps], axis=0)
            put(lpart, ps, at, value)
            gains = value * rows_of(normed, ps, at).astype(F32)
            gain_acc[:, at] += gains.reshape(-1, 8, wt).sum(axis=0)
            return carry

        lax.fori_loop(0, width // wt, outs, 0, unroll=True)
        summed.pair_send(i)

    def ring_start(q, lhs, ring):
        some_terms(q, lhs, normed, TERMS, 0, 2)
        ring.ready(2, 1)
        ring.ready(2, 0)
        some_terms(q, lhs, normed, TERMS, 2, 4)
        ring.ready(1, 0)
        ring.ready(3, 1)

    weigh(ggt)
    ring_start(0, ggt, gate_sum)
    weigh(hid_t)
    some_terms(2, hid_t, again, DOWN, 0, 4)
    for off in (2, 1, 3, 0):
        down_sum.ready(off, 1)
    weigh(ugt)
    ring_start(1, ugt, up_sum)
    frozen.w.drain(most, sib)
    o_scores[...] = flat_scores[...].T[:1]
    columns = jnp.concatenate([row_w[k] for k in range(16)], axis=0).T
    for p in range(8):
        both = columns[:, 2 * p : 2 * p + 1] + columns[:, 2 * p + 1 : 2 * p + 2]
        col_w[p] = jnp.broadcast_to(both, col_w.shape[1:])
    normed_part(0)
    normed_part(1)
    summed.ready(0)
    normed_part(2)
    summed.ready(1)
    normed_part(3)
    summed.ready(2)
    gain_t[s.t] = jnp.sum(gain_acc[...], axis=0, keepdims=True) / lgain[...]
    tw, pw = Wires(tsend.at[0], trecv), Wires(psend.at[0], precv)
    for r in range(1, 16):
        tw.send(gain_t.at[s.t], gain_t.at[s.t], 0, 0, {"tensor": (s.t + r) % 16})
    some_terms(0, ggt, normed, TERMS, 4, 8)
    gate_sum.stage2()
    summed.ready(3)
    summed.a.stage2()
    summed.b.stage2()
    some_terms(1, ugt, normed, TERMS, 4, 8)
    some_terms(2, hid_t, again, DOWN, 4, 8)
    up_sum.stage2()
    down_sum.far_out()
    down_sum.near_out()
    summed.a.stage3()
    summed.b.stage3()
    tw.got(gain_t.at[pl.ds(0, 15)], 0, sib)
    gain_d[d] = jnp.sum(gain_t[...], axis=0)
    for r in range(1, 8):
        pw.send(gain_d.at[d], gain_d.at[d], 0, 0, {"dp": (d + r) % 8})
    gate_sum.stage3()
    up_sum.stage3()
    down_sum.stage3()

    def token_grads(nrefs, base):
        def rows(k, carry):
            at = pl.ds(pl.multiple_of(k * ROWS, ROWS), ROWS)
            here = pl.ds(pl.multiple_of(base + k * ROWS, ROWS), ROWS)
            v = tokens[here].astype(F32)
            inv = lax.rsqrt(jnp.mean(v * v, axis=-1, keepdims=True) + 1e-05)
            scaled = total_of(nrefs, at) * lgain[...]
            mid = jnp.mean(scaled * v, axis=-1, keepdims=True)
            o_tokens[here] = (inv * scaled - v * (inv * inv * inv * mid)).astype(BF16)
            return carry

        lax.fori_loop(0, block // 2 // ROWS, rows, 0)

    token_grads(summed.a.stage4(), 0)
    token_grads(summed.b.stage4(), block // 2)
    emit(o_tokens, grad_tokens)
    pw.got(gain_d.at[pl.ds(0, 7)], 0, sib)
    o_gain[...] = jnp.sum(gain_d[...], axis=0)
    emit(o_gain, grad_gain)
    emit(o_scores, scores)

    def finish_plain(out, refs):
        def rows(k, carry):
            at = pl.ds(pl.multiple_of(k * ROWS, ROWS), ROWS)
            out[at] = total_of(refs, at)
            return carry

        lax.fori_loop(0, hidden // ROWS, rows, 0)

    def finish_turned(out, refs):
        def rows(k, carry):
            at = tile(k, 128)
            out[:, at] = total_of(refs, at).T
            return carry

        lax.fori_loop(0, hidden // 128, rows, 0)

    finish_turned(o_gate, gate_sum.stage4())
    emit(o_gate, out_gate)
    finish_turned(o_up, up_sum.stage4())
    emit(o_up, out_up)
    finish_plain(o_down, down_sum.stage4())
    emit(o_down, out_down)
    for wires, ref in (
        (summed.w, most),
        (regather.w, most),
        (gate_sum.w, terms.at[0, pl.ds(0, 7)]),
        (up_sum.w, terms.at[1, pl.ds(0, 7)]),
        (down_sum.w, terms.at[2, pl.ds(0, 7)]),
        (tw, gain_t.at[pl.ds(0, 15)]),
        (pw, gain_d.at[pl.ds(0, 7)]),
        (ww, row_w.at[pl.ds(0, 15)]),
    ):
        wires.drain(ref, sib)
    for copy in outs:
        copy.wait()


def hand_over(count, *refs):
    srcs, dsts, held, sems = refs[:count], refs[count : 2 * count], refs[2 * count : -1], refs[-1]
    ins = [pltpu.make_async_copy(a, b, sems.at[0, k]) for k, (a, b) in enumerate(zip(srcs, held))]
    outs = [pltpu.make_async_copy(a, b, sems.at[1, k]) for k, (a, b) in enumerate(zip(held, dsts))]
    for copy in ins:
        copy.start()
    for copy, then in zip(ins, outs):
        copy.wait()
        then.start()
    for copy in outs:
        copy.wait()


def local(
    tokens, targets, learner_gain, learner_gate, learner_up, learner_down,
    frozen_gain, frozen_gate, frozen_up, frozen_down,
):
    block, width = tokens.shape
    hidden = learner_gate.shape[1]
    cut, group, half = width // 8, 16 * block, block // 2
    away = pl.BlockSpec(memory_space=pl.ANY)
    shape, vmem = jax.ShapeDtypeStruct, pltpu.VMEM

    def dma(*counts):
        return [pltpu.SemaphoreType.DMA((k,)) for k in counts]

    def twice(*shapes):
        return [vmem((*lead, width), BF16) for lead in shapes for _ in range(2)]

    blocks = vmem((8, 2, block, width), BF16)
    pre = vmem((8, 2 * block, hidden), F32)
    flat = vmem((8, 2 * block, hidden), BF16)
    turned = vmem((hidden, group), BF16)
    ring, mine = vmem((6, hidden, cut), BF16), vmem((hidden, cut), BF16)
    shapes = (
        shape((1, block), F32),
        shape((block, width), BF16),
        shape((1, width), F32),
        shape((cut, hidden), F32),
        shape((cut, hidden), F32),
        shape((hidden, cut), F32),
    )
    held = [vmem(a.shape, a.dtype) for a in shapes]
    results = pl.pallas_call(
        kernel,
        out_shape=shapes,
        in_specs=[away] * 10,
        out_specs=[away] * 6,
        scratch_shapes=[blocks, blocks, vmem((2, 2, block, width), BF16), pre, pre, turned]
        + [vmem((4 * block, hidden), BF16), blocks, blocks]
        + twice((8, block), (6, half), (half,), (4, half), (2, half // 2), (2, half))
        + [blocks, vmem((6, half, width), BF16), vmem((half, width), BF16)]
        + [vmem((2 * block, 128), F32), vmem((16, 1, 128), F32), vmem((8, 2 * block, 128), F32)]
        + [vmem((block, width), BF16)] * 2
        + [vmem((1, width), F32)] * 2
        + [vmem((width, hidden), BF16)] * 2
        + [vmem((hidden, width), BF16), vmem((3, 8, hidden, cut), BF16)]
        + [vmem((block, width), BF16), vmem((block, 128), F32), flat, flat, turned, turned]
        + [ring, mine, ring, mine]
        + [vmem((k, hidden // h, cut), BF16) for k, h in ((4, 1), (2, 2), (2, 1))]
        + [vmem((8, width), F32), vmem((16, 1, width), F32), vmem((8, 1, width), F32)]
        + held
        + dma(10, 6, 1, 25, 1, 25, 1, 25, 2, 14, 1, 10, 1, 1, 1, 1, 1, 1),
        compiler_params=pltpu.CompilerParams(
            has_side_effects=True, vmem_limit_bytes=VMEM_LIMIT, collective_id=1
        ),
        name="step",
    )(
        tokens, targets, learner_gain.reshape(1, width), frozen_gain.reshape(1, width),
        learner_gate, learner_up, learner_down, frozen_gate, frozen_up, frozen_down,
    )
    scores, grad_tokens, grad_gain, grad_gate, grad_up, grad_down = pl.pallas_call(
        functools.partial(hand_over, len(shapes)),
        out_shape=shapes,
        in_specs=[away] * 6,
        out_specs=[away] * 6,
        scratch_shapes=held + [pltpu.SemaphoreType.DMA((2, 6))],
        name="hand_over",
    )(*results)
    return (
        scores.reshape(block),
        grad_tokens,
        grad_gain.reshape(width),
        grad_gate,
        grad_up,
        grad_down,
    )


def solution(mesh):
    placed = (
        P(("dp", "tensor"), None),
        P(("dp", "tensor"), None),
        P(),
        P(None, "tensor"),
        P(None, "tensor"),
        P("tensor", None),
        P(),
        P(None, "tensor"),
        P(None, "tensor"),
        P("tensor", None),
    )
    return jax.shard_map(
        local,
        mesh=mesh,
        in_specs=placed,
        out_specs=(
            P(("dp", "tensor")),
            P(("dp", "tensor"), None),
            P(),
            P("dp", "tensor"),
            P("dp", "tensor"),
            P("tensor", "dp"),
        ),
        check_vma=False,
    )
```
